256 devices in a mesh: feat: 8 (over y, core), dom: 32 (over x, z).
Axes of the slice: x: 4, y: 4, z: 8, core: 2. Of those that a mesh axis runs over, the one named last changes fastest.
Arguments:
- features: bfloat16 [131072, 128], P('dom'), may hold values from -6 to 6
- w_input: bfloat16 [128, 256], P(None, 'feat'), may hold values from -0.5 to 0.5
- layer_weights: bfloat16 [4, 256, 256], replicated, may hold values from -0.375 to 0.375
- history: bfloat16 [4, 131072, 256], P(None, 'dom', 'feat'), may hold values from 0 to 2
- tile_values: bfloat16 [1024, 6, 128, 128], P('dom'), may hold values from -0.21875 to 0.21875
- tile_columns: int32 [1024, 6], P('dom'), may hold values from 0 to 159, as said below
- send_rows: int32 [32, 32, 512], P('dom'), may hold values from 0 to 4095
- send_counts: int32 [32, 32], P('dom'), may hold values from 0 to 512, as said below
Outputs:
- pushed: bfloat16 [4, 131072, 256], P(None, 'dom', 'feat')
- final_rows: bfloat16 [131072, 256], P('dom', 'feat')
The draws below stay inside these ranges and needn't reach their ends.
Inputs may be any that keep to these rules, and one draw needn't show every extreme that they name: `tile_columns`: per row of tiles the first 2 entries lie below 4096 / 128 (own rows), the others at or above it (halo slots); every halo column tile of every partition is named somewhere. `send_counts`: A partition sends nothing to itself; in every draw some destination receives exactly 512 rows from every other partition.
All inputs are finite; a program needn't handle non-finite values.
Results may differ from the reference program's by a relative error of at most 0.0052.
Values may be sent and summed in bfloat16 or wider, within the bound.
A program may use at most 128 MiB of HBM per device.

```python
import math
import jax
import jax.numpy as jnp
from jax import lax

F = 256
IN_FEAT = 128
NODES_DEV = 4096
CAP = 512
TILE = 128
K = 6
K_LOC = 2
LAYERS = 4
NODES = 131072
HALO = 16384
ROW_TILES = 1024
N_DOM = 32


def shuffle_one(sub_key, span):
    return jax.random.permutation(sub_key, span)


def draw_tile_columns(key, part):
    local_tiles = NODES_DEV // TILE
    halo_tiles = HALO // TILE
    remote_count = K - K_LOC
    key_local, key_shuffle = jax.random.split(key)
    local_cols = jax.random.randint(key_local, (ROW_TILES, K_LOC), 0, local_tiles)
    block_keys = jax.random.split(key_shuffle, N_DOM)
    span = local_tiles * remote_count
    shuffled = jax.vmap(lambda sub_key: shuffle_one(sub_key, span))(block_keys)
    remote = local_tiles + shuffled % halo_tiles
    remote = remote.reshape(ROW_TILES, remote_count)
    return jnp.concatenate([local_cols, remote], axis=1).astype(jnp.int32)


def draw_send_counts(key, part):
    key_heavy, key_high, key_low, key_busy = jax.random.split(key, 4)
    dest_ids = jnp.arange(N_DOM)
    busiest = jax.random.randint(key_busy, (), 0, N_DOM)
    heavy_dest = (jax.random.randint(key_heavy, (N_DOM,), 0, 4) == 0) | (dest_ids == busiest)
    high_counts = jax.random.randint(key_high, (N_DOM, N_DOM), CAP // 2, CAP + 1)
    low_counts = jax.random.randint(key_low, (N_DOM, N_DOM), (CAP + 7) // 8, CAP // 2 + 1)
    counts = jnp.where(heavy_dest[None, :], high_counts, low_counts)
    counts = jnp.where(dest_ids[None, :] == busiest, CAP, counts)
    counts = jnp.where(dest_ids[:, None] == dest_ids[None, :], 0, counts)
    return counts.astype(jnp.int32)


def touch_ends(drawn, rng, low, top_value):
    place = [jax.random.randint(jax.random.fold_in(rng, axis), (), 0, length) for axis, length in enumerate(drawn.shape)]
    main_axis = drawn.shape.index(max(drawn.shape))
    neighbour = place[:main_axis] + [(place[main_axis] + 1) % drawn.shape[main_axis]] + place[main_axis + 1:]
    return drawn.at[tuple(place)].set(low).at[tuple(neighbour)].set(top_value)


def shard_levels(rng, extent, shards, least, largest):
    gain = 1.0
    for dim, parts in shards:
        draws = jax.random.uniform(jax.random.fold_in(jax.random.fold_in(rng, 6), dim), (parts,), jnp.float32, least / len(shards), largest / len(shards))
        gain = gain * jnp.repeat(jnp.exp(draws), extent[dim] // parts).reshape((-1,) + (1,) * (len(extent) - 1 - dim))
    return gain


def normal_values(key, dims, spread, reach, pieces=(), kind=jnp.bfloat16):
    drawn = jax.random.normal(key, dims, jnp.float32) * spread
    if len(pieces) > 0:
        drawn = shard_levels(key, dims, pieces, -0.22, 0.18) * drawn
    return jnp.clip(drawn, min=-reach, max=reach).astype(kind)


def setup_inputs(seed: int = 0) -> dict:
    splits = jax.random.split(jax.random.key(seed), 9)
    features = normal_values(splits[0], (NODES, IN_FEAT), 1.0, 6.0, ((0, 32),))
    w_input = normal_values(splits[1], (IN_FEAT, F), IN_FEAT ** -0.5, 0.5, ((1, 8),))
    layer_weights = normal_values(splits[2], (LAYERS, F, F), F ** -0.5, 0.375)
    history = jnp.clip(2.0 * jax.random.uniform(splits[3], (LAYERS, NODES, F), jnp.float32) ** shard_levels(splits[3], (LAYERS, NODES, F), ((1, 32), (2, 8)), -0.2, 0.2), 0.0, 2.0).astype(jnp.bfloat16)
    tile_values = normal_values(splits[4], (ROW_TILES, K, TILE, TILE), (K * TILE) ** -0.5, 0.21875, ((0, 32),))
    tile_columns = draw_tile_columns(jax.random.fold_in(splits[8], 71), 0)
    send_rows = touch_ends(jax.random.randint(splits[6], (N_DOM, N_DOM, CAP), 0, NODES_DEV), jax.random.fold_in(splits[6], 1), 0, NODES_DEV - 1).astype(jnp.int32)
    send_counts = draw_send_counts(jax.random.fold_in(splits[8], 71), 0)
    return dict(features=features, w_input=w_input, layer_weights=layer_weights, history=history, tile_values=tile_values, tile_columns=tile_columns, send_rows=send_rows, send_counts=send_counts)


ALPHA = 0.1
LAMBDA_DECAY = 0.5


def reference(features, w_input, layer_weights, history, tile_values, tile_columns, send_rows, send_counts):
    initial = jnp.maximum(jnp.dot(features, w_input, preferred_element_type=jnp.float32), 0.0).astype(jnp.bfloat16)
    slot_ids = jnp.arange(CAP)
    sources = jnp.arange(N_DOM)
    local_tiles = NODES_DEV // TILE
    pushed = []
    current = initial
    for layer_index in range(LAYERS):
        beta_layer = math.log(LAMBDA_DECAY / (layer_index + 1) + 1.0)
        layer_table = history[layer_index]

        def one_part(part_index):
            source_rows = sources[:, None] * NODES_DEV + send_rows[:, part_index, :]
            live_mask = slot_ids[None, :] < send_counts[:, part_index][:, None]
            halo_rows = jnp.where(live_mask[:, :, None], layer_table[source_rows], jnp.zeros((), jnp.bfloat16))
            halo_rows = halo_rows.reshape(N_DOM * CAP, F)
            own_rows = lax.dynamic_slice_in_dim(current, (part_index * NODES_DEV).astype(jnp.int32), NODES_DEV, 0)
            combined = jnp.concatenate([own_rows, halo_rows], axis=0).reshape(-1, TILE, F)
            columns = lax.dynamic_slice_in_dim(tile_columns, (part_index * local_tiles).astype(jnp.int32), local_tiles, 0)
            values = lax.dynamic_slice_in_dim(tile_values, (part_index * local_tiles).astype(jnp.int32), local_tiles, 0)
            picked = combined[columns]
            summed = jnp.einsum('rkab,rkbf->raf', values.astype(jnp.float32), picked.astype(jnp.float32))
            return summed.reshape(NODES_DEV, F)

        aggregated = lax.map(one_part, jnp.arange(N_DOM, dtype=jnp.int32)).reshape(NODES, F)
        blended = ((1.0 - ALPHA) * aggregated + ALPHA * initial.astype(jnp.float32)).astype(jnp.bfloat16)
        blended = lax.optimization_barrier(blended)
        product = jnp.dot(blended, layer_weights[layer_index], preferred_element_type=jnp.float32)
        fresh = jnp.maximum((1.0 - beta_layer) * blended.astype(jnp.float32) + beta_layer * product, 0.0)
        pushed.append(current)
        current = fresh.astype(jnp.bfloat16)
    return jnp.stack(pushed), current
```

```python
import functools
import math

import jax
import jax.numpy as jnp
from jax import lax
from jax.experimental import pallas as pl
from jax.experimental.pallas import tpu as pltpu
from jax.sharding import PartitionSpec as P

MESH = pl.DeviceIdType.MESH
LAYERS = 4
ALPHA = 0.1
LAMBDA_DECAY = 0.5
TILE = 128
LANES = 128
PACK = 4
WIDTH = 32
NFEAT = 8
GROUPS = 8
CAP = 512
NODES_DEV = 4096
F = 256
K = 6
BF = jnp.bfloat16
F32 = jnp.float32


def lane_ids(rows):
    return lax.broadcasted_iota(jnp.int32, (rows, LANES), 1)


def swap_blocks(parts):
    x0, x1, x2, x3 = parts
    lane = lane_ids(x0.shape[0])
    low = lane < 64
    even = (lane & 32) == 0
    a0 = jnp.where(low, x0, pltpu.roll(x2, 64, 1))
    a2 = jnp.where(low, pltpu.roll(x0, 64, 1), x2)
    a1 = jnp.where(low, x1, pltpu.roll(x3, 64, 1))
    a3 = jnp.where(low, pltpu.roll(x1, 64, 1), x3)
    y0 = jnp.where(even, a0, pltpu.roll(a1, 32, 1))
    y1 = jnp.where(even, pltpu.roll(a0, 96, 1), a1)
    y2 = jnp.where(even, a2, pltpu.roll(a3, 32, 1))
    y3 = jnp.where(even, pltpu.roll(a2, 96, 1), a3)
    return y0, y1, y2, y3


def fill_table(table_t, table):
    def block(i, carry):
        start = pl.multiple_of(i * TILE, TILE)
        part = table_t[:, pl.ds(start, TILE)].astype(F32)
        table[pl.ds(start, TILE), :] = part.T
        return carry

    lax.fori_loop(0, NODES_DEV // TILE, block, 0)
    table[pl.ds(NODES_DEV, 8), :] = jnp.zeros((8, LANES), F32)


def gather_rows(rows, table, picked, dest):
    for j in range(CAP):
        picked[pl.ds(j, 1), :] = table[pl.ds(rows[dest, j], 1), :]


def pack_rows(picked, packed, dest):
    for c in range(4):
        parts = [picked[pl.ds(t * TILE + c * 32, 32), :] for t in range(PACK)]
        for level, part in enumerate(swap_blocks(parts)):
            packed[level, dest, pl.ds(c * 32, 32), :] = part.astype(BF)


def gather_kernel(n_dom, rows, table_t, packed, table, picked):
    fill_table(table_t, table)

    def one(dest, carry):
        gather_rows(rows, table, picked, dest)
        pack_rows(picked, packed, dest)
        return carry

    lax.fori_loop(0, n_dom, one, 0)


def layer_kernel(
    n_dom, grid_x, grid_z,
    group_ref, block_ref, packed, feats_hbm, w_in, values_hbm, weights, masks,
    pushed, final,
    comb0, comb1, comb2, comb3, last, initial, feats, values, zs, zr, hs,
    load_sem, dom_send, dom_recv, z_send, z_recv, h_send, h_recv,
):
    comb = (comb0, comb1, comb2, comb3, last)
    f_me = lax.axis_index("feat")
    d_me = lax.axis_index("dom")
    x_me, z_me = d_me // grid_z, d_me % grid_z

    barrier = pltpu.get_barrier_semaphore()

    def greet_dom(i, carry):
        pl.semaphore_signal(
            barrier, inc=1, device_id=(f_me, lax.rem(d_me + 1 + i, n_dom)), device_id_type=MESH
        )
        return carry

    def greet_feat(i, carry):
        pl.semaphore_signal(
            barrier, inc=1, device_id=(lax.rem(f_me + 1 + i, NFEAT), d_me), device_id_type=MESH
        )
        return carry

    lax.fori_loop(0, n_dom - 1, greet_dom, 0)
    lax.fori_loop(0, NFEAT - 1, greet_feat, 0)
    load_feats = pltpu.make_async_copy(feats_hbm, feats, load_sem.at[0])
    load_values = pltpu.make_async_copy(values_hbm, values, load_sem.at[1])
    load_feats.start()
    load_values.start()
    pl.semaphore_wait(barrier, n_dom - 1 + NFEAT - 1)

    def dom_copy(level, k):
        i = lax.rem(k, grid_z)
        half = grid_z // 2
        dz = jnp.where(lax.rem(i, 2) == 1, half - (i + 1) // 2, half + i // 2)
        dx = lax.rem(grid_x - 1 - k // grid_z + i + 1, grid_x)
        dest = lax.rem(x_me + dx, grid_x) * grid_z + lax.rem(z_me + dz, grid_z)
        return pltpu.make_async_remote_copy(
            src_ref=packed.at[level, dest],
            dst_ref=comb[level].at[GROUPS + d_me],
            send_sem=dom_send.at[level, k],
            recv_sem=dom_recv.at[level, k],
            device_id=(f_me, dest),
            device_id_type=MESH,
        )

    def send_level(level):
        def one(k, carry):
            dom_copy(level, k).start()
            return carry

        lax.fori_loop(0, n_dom - 1, one, 0)

    def wait_level(level):
        def one(k, carry):
            dom_copy(level, k).wait_recv()
            return carry

        lax.fori_loop(0, n_dom - 1, one, 0)

    def feat_copy(source, target, send_sem, recv_sem, i):
        dest = lax.rem(f_me + 1 + i, NFEAT)
        return pltpu.make_async_remote_copy(
            src_ref=source.at[dest],
            dst_ref=target.at[f_me],
            send_sem=send_sem.at[i],
            recv_sem=recv_sem.at[i],
            device_id=(dest, d_me),
            device_id_type=MESH,
        )

    send_level(0)
    send_level(1)
    for level in range(LAYERS):
        comb[level][GROUPS + d_me] = jnp.zeros((TILE, LANES), BF)

    load_feats.wait()

    def start_group(g, carry):
        for c in range(2):
            rows = [
                feats[pl.ds(pl.multiple_of((g * PACK + t) * TILE + c * 64, 64), 64), :]
                for t in range(PACK)
            ]
            h0 = jnp.dot(jnp.concatenate(rows, axis=1), w_in[...], preferred_element_type=F32)
            h0 = jnp.maximum(h0, 0.0).astype(BF)
            comb0[g, pl.ds(c * 64, 64), :] = h0
            initial[g, pl.ds(c * 64, 64), :] = h0
        return carry

    lax.fori_loop(0, GROUPS, start_group, 0)
    load_values.wait()

    def emit_rows(level, target):
        def one(g, carry):
            flipped = comb[level][g].astype(F32).T.astype(BF)
            for t in range(PACK):
                start = pl.multiple_of((g * PACK + t) * TILE, TILE)
                target(flipped[t * WIDTH:(t + 1) * WIDTH], start)
            return carry

        lax.fori_loop(0, GROUPS, one, 0)

    for level in range(LAYERS):
        beta = math.log(LAMBDA_DECAY / (level + 1) + 1.0)
        wait_level(level)
        if level + 2 < LAYERS:
            send_level(level + 2)

        def propagate(i, carry):
            g = lax.rem(f_me + 1 + i, GROUPS)
            lane = lane_ids(TILE)
            agg = jnp.zeros((TILE, LANES), F32)
            for t in range(PACK):
                r = g * PACK + t
                picked = []
                for k in range(K):
                    tile = comb[level][group_ref[r, k]]
                    picked.append(tile * masks[block_ref[r, k]])
                lhs = jnp.concatenate([values[r, k] for k in range(K)], axis=1)
                out = jnp.dot(
                    lhs, jnp.concatenate(picked, axis=0), preferred_element_type=F32
                )
                out = out + pltpu.roll(out, 64, 1)
                out = out + pltpu.roll(out, 32, 1)
                agg = jnp.where((lane >> 5) == t, out, agg)
            z = (1.0 - ALPHA) * agg + ALPHA * initial[g].astype(F32)
            zs[level, g] = z.astype(BF)
            return carry

        def send_z(i):
            feat_copy(zs.at[level], zr.at[level], z_send.at[level], z_recv.at[level], i).start()

        def step(i, carry):
            propagate(i, 0)
            send_z(i - 1)
            return carry

        propagate(0, 0)
        lax.fori_loop(1, NFEAT, step, 0)
        zr[level, f_me] = zs[level, f_me]

        def push(part, start):
            pushed[level, :, pl.ds(start, TILE)] = part

        emit_rows(level, push)

        def wait_z(i, carry):
            feat_copy(
                zs.at[level], zr.at[level], z_send.at[level], z_recv.at[level], i
            ).wait_recv()
            return carry

        lax.fori_loop(0, NFEAT - 1, wait_z, 0)

        def mix(c, carry):
            start = pl.multiple_of(c * 32, 32)
            parts = [zr[level, f, pl.ds(start, 32), :].astype(F32) for f in range(NFEAT)]
            left = swap_blocks(parts[:4])
            right = swap_blocks(parts[4:])
            block = jnp.concatenate(
                [jnp.concatenate([left[t], right[t]], axis=1) for t in range(PACK)], axis=0
            )
            product = jnp.dot(block.astype(BF), weights[level], preferred_element_type=F32)
            fresh = jnp.maximum((1.0 - beta) * block + beta * product, 0.0)
            for a in range(2):
                outs = swap_blocks(
                    [fresh[t * 32:(t + 1) * 32, a * LANES:(a + 1) * LANES] for t in range(PACK)]
                )
                for b in range(PACK):
                    hs[level, a * PACK + b, pl.ds(start, 32), :] = outs[b].astype(BF)
            return carry

        lax.fori_loop(0, 4, mix, 0)
        comb[level + 1][f_me] = hs[level, f_me]

        def send_h(i, carry):
            feat_copy(
                hs.at[level], comb[level + 1], h_send.at[level], h_recv.at[level], i
            ).start()
            return carry

        def wait_h(i, carry):
            feat_copy(
                hs.at[level], comb[level + 1], h_send.at[level], h_recv.at[level], i
            ).wait_recv()
            return carry

        lax.fori_loop(0, NFEAT - 1, send_h, 0)
        lax.fori_loop(0, NFEAT - 1, wait_h, 0)

    def finish(part, start):
        final[:, pl.ds(start, TILE)] = part

    emit_rows(LAYERS, finish)

    for level in range(LAYERS):
        def drain_dom(k, carry):
            dom_copy(level, k).wait_send()
            return carry

        def drain_feat(i, carry):
            feat_copy(
                zs.at[level], zr.at[level], z_send.at[level], z_recv.at[level], i
            ).wait_send()
            feat_copy(
                hs.at[level], comb[level + 1], h_send.at[level], h_recv.at[level], i
            ).wait_send()
            return carry

        lax.fori_loop(0, n_dom - 1, drain_dom, 0)
        lax.fori_loop(0, NFEAT - 1, drain_feat, 0)


def on_device(
    n_dom, features, w_input, layer_weights, history, tile_values, tile_columns, send_rows, send_counts
):
    grid_x, grid_z = (4, 8) if n_dom == 32 else (1, n_dom)
    live = jnp.arange(CAP)[None, :] < send_counts[0][:, None]
    rows = jnp.where(live, send_rows[0], NODES_DEV)
    table_t = history.transpose(0, 2, 1).reshape(LAYERS * WIDTH, NODES_DEV)
    vmem = pl.BlockSpec(memory_space=pltpu.VMEM)
    smem = pl.BlockSpec(memory_space=pltpu.SMEM)
    hbm = pl.BlockSpec(memory_space=pl.ANY)
    packed = pl.pallas_call(
        functools.partial(gather_kernel, n_dom),
        out_shape=jax.ShapeDtypeStruct((LAYERS, n_dom, TILE, LANES), BF),
        in_specs=[smem, vmem],
        out_specs=vmem,
        scratch_shapes=[
            pltpu.VMEM((NODES_DEV + 8, LANES), F32),
            pltpu.VMEM((CAP, LANES), F32),
        ],
        name="gather_halo",
    )(rows, table_t)

    zero = jnp.zeros_like(w_input)
    w_in = jnp.concatenate(
        [
            jnp.concatenate([w_input if a == t else zero for a in range(PACK)], axis=1)
            for t in range(PACK)
        ],
        axis=0,
    )
    masks = (
        jnp.arange(LANES)[None, None, :] // WIDTH == jnp.arange(PACK)[:, None, None]
    ).astype(BF)
    masks = jnp.broadcast_to(masks, (PACK, TILE, LANES))
    sem = pltpu.SemaphoreType.DMA
    pushed, final = pl.pallas_call(
        functools.partial(layer_kernel, n_dom, grid_x, grid_z),
        out_shape=(
            jax.ShapeDtypeStruct((LAYERS, WIDTH, NODES_DEV), BF),
            jax.ShapeDtypeStruct((WIDTH, NODES_DEV), BF),
        ),
        in_specs=[smem, smem, hbm, hbm, vmem, hbm, vmem, vmem],
        out_specs=(vmem, vmem),
        scratch_shapes=[
            *[pltpu.VMEM((GROUPS + n_dom, TILE, LANES), BF) for _ in range(LAYERS)],
            pltpu.VMEM((GROUPS, TILE, LANES), BF),
            pltpu.VMEM((GROUPS, TILE, LANES), BF),
            pltpu.VMEM((NODES_DEV, LANES), BF),
            pltpu.VMEM((NODES_DEV // TILE, K, TILE, TILE), BF),
            pltpu.VMEM((LAYERS, NFEAT, TILE, LANES), BF),
            pltpu.VMEM((LAYERS, NFEAT, TILE, LANES), BF),
            pltpu.VMEM((LAYERS, NFEAT, TILE, LANES), BF),
            sem((2,)),
            sem((LAYERS, n_dom - 1)),
            sem((LAYERS, n_dom - 1)),
            sem((LAYERS, NFEAT - 1)),
            sem((LAYERS, NFEAT - 1)),
            sem((LAYERS, NFEAT - 1)),
            sem((LAYERS, NFEAT - 1)),
        ],
        compiler_params=pltpu.CompilerParams(collective_id=0, has_side_effects=True),
        name="halo_layers",
    )(
        tile_columns // PACK, tile_columns % PACK, packed, features, w_in, tile_values,
        layer_weights, masks,
    )
    return pushed.transpose(0, 2, 1), final.transpose(1, 0)


def solution(mesh):
    placed = (
        P("dom", None),
        P(None, "feat"),
        P(),
        P(None, "dom", "feat"),
        P("dom", None, None, None),
        P("dom", None),
        P("dom", None, None),
        P("dom", None),
    )
    return jax.shard_map(
        functools.partial(on_device, mesh.shape["dom"]),
        mesh=mesh,
        in_specs=placed,
        out_specs=(P(None, "dom", "feat"), P("dom", "feat")),
        check_vma=False,
    )
```

```python
import functools
import math

import jax
import jax.numpy as jnp
from jax import lax
from jax.experimental import pallas as pl
from jax.experimental.pallas import tpu as pltpu
from jax.sharding import PartitionSpec as P

MESH = pl.DeviceIdType.MESH
LAYERS = 4
ALPHA = 0.1
LAMBDA_DECAY = 0.5
TILE = 128
LANES = 128
PACK = 4
WIDTH = 32
NFEAT = 8
GROUPS = 8
CAP = 512
NODES_DEV = 4096
F = 256
K = 6
BF = jnp.bfloat16
F32 = jnp.float32


def lane_ids(rows):
    return lax.broadcasted_iota(jnp.int32, (rows, LANES), 1)


def swap_blocks(parts):
    x0, x1, x2, x3 = parts
    lane = lane_ids(x0.shape[0])
    low = lane < 64
    even = (lane & 32) == 0
    a0 = jnp.where(low, x0, pltpu.roll(x2, 64, 1))
    a2 = jnp.where(low, pltpu.roll(x0, 64, 1), x2)
    a1 = jnp.where(low, x1, pltpu.roll(x3, 64, 1))
    a3 = jnp.where(low, pltpu.roll(x1, 64, 1), x3)
    y0 = jnp.where(even, a0, pltpu.roll(a1, 32, 1))
    y1 = jnp.where(even, pltpu.roll(a0, 96, 1), a1)
    y2 = jnp.where(even, a2, pltpu.roll(a3, 32, 1))
    y3 = jnp.where(even, pltpu.roll(a2, 96, 1), a3)
    return y0, y1, y2, y3


def fill_table(table_t, table):
    def block(i, carry):
        start = pl.multiple_of(i * TILE, TILE)
        table[pl.ds(start, TILE), :] = table_t[:, pl.ds(start, TILE)].astype(F32).T
        return carry

    lax.fori_loop(0, NODES_DEV // TILE, block, 0)


def gather_rows(rows, table, picked, dest):
    base = dest * CAP
    for j in range(CAP):
        picked[pl.ds(j, 1), :] = table[pl.ds(rows[base + j], 1), :]


def pack_rows(counts, picked, packed, dest):
    row = lax.broadcasted_iota(jnp.int32, (32, LANES), 0)
    count = counts[0, dest]
    for c in range(4):
        parts = []
        for t in range(PACK):
            start = t * TILE + c * 32
            live = row < count - start
            parts.append(jnp.where(live, picked[pl.ds(start, 32), :], 0.0))
        for level, part in enumerate(swap_blocks(parts)):
            packed[level, dest, pl.ds(c * 32, 32), :] = part.astype(BF)


def layer_kernel(
    n_dom, grid_x, grid_z,
    columns, rows, counts, table_hbm, feats_hbm, w_in_t, values_hbm, weights_hbm,
    pushed, final,
    table_t, table, picked, packed, masks, w_wide,
    comb0, comb1, comb2, comb3, last, initial, feats, values, weights, zs, zr, hs,
    load_sem, dom_send, dom_recv, z_send, z_recv, h_send, h_recv,
):
    comb = (comb0, comb1, comb2, comb3, last)
    f_me = lax.axis_index("feat")
    d_me = lax.axis_index("dom")
    x_me, z_me = d_me // grid_z, d_me % grid_z

    barrier = pltpu.get_barrier_semaphore()

    def greet_dom(i, carry):
        pl.semaphore_signal(
            barrier, inc=1, device_id=(f_me, lax.rem(d_me + 1 + i, n_dom)), device_id_type=MESH
        )
        return carry

    def greet_feat(i, carry):
        pl.semaphore_signal(
            barrier, inc=1, device_id=(lax.rem(f_me + 1 + i, NFEAT), d_me), device_id_type=MESH
        )
        return carry

    lax.fori_loop(0, n_dom - 1, greet_dom, 0)
    lax.fori_loop(0, NFEAT - 1, greet_feat, 0)
    load_table = pltpu.make_async_copy(table_hbm, table_t, load_sem.at[0])
    load_feats = pltpu.make_async_copy(feats_hbm, feats, load_sem.at[1])
    load_values = pltpu.make_async_copy(values_hbm, values, load_sem.at[2])
    load_weights = pltpu.make_async_copy(weights_hbm, weights, load_sem.at[3])
    load_table.start()
    load_feats.start()
    load_values.start()
    load_weights.start()
    lane = lane_ids(TILE)
    for b in range(PACK):
        masks[b] = jnp.where((lane >> 5) == b, 1.0, 0.0).astype(BF)
    w_wide[...] = jnp.zeros((LANES, PACK * TILE), BF)
    for t in range(PACK):
        w_wide[t * WIDTH:(t + 1) * WIDTH, t * TILE:(t + 1) * TILE] = w_in_t[...]
    load_table.wait()
    fill_table(table_t, table)
    pl.semaphore_wait(barrier, n_dom - 1 + NFEAT - 1)

    def dest_of(k):
        i = lax.rem(k, grid_z)
        half = grid_z // 2
        dz = jnp.where(lax.rem(i, 2) == 1, half - (i + 1) // 2, half + i // 2)
        dx = lax.rem(grid_x - 1 - k // grid_z + i + 1, grid_x)
        return lax.rem(x_me + dx, grid_x) * grid_z + lax.rem(z_me + dz, grid_z)

    def dom_copy(level, k):
        dest = dest_of(k)
        return pltpu.make_async_remote_copy(
            src_ref=packed.at[level, dest],
            dst_ref=comb[level].at[GROUPS + d_me],
            send_sem=dom_send.at[level, k],
            recv_sem=dom_recv.at[level, k],
            device_id=(f_me, dest),
            device_id_type=MESH,
        )

    def send_level(level):
        def one(k, carry):
            dom_copy(level, k).start()
            return carry

        lax.fori_loop(0, n_dom - 1, one, 0)

    def wait_level(level):
        def one(k, carry):
            dom_copy(level, k).wait_recv()
            return carry

        lax.fori_loop(0, n_dom - 1, one, 0)

    def feat_copy(source, target, send_sem, recv_sem, i):
        dest = lax.rem(f_me + 1 + i, NFEAT)
        return pltpu.make_async_remote_copy(
            src_ref=source.at[dest],
            dst_ref=target.at[f_me],
            send_sem=send_sem.at[i],
            recv_sem=recv_sem.at[i],
            device_id=(dest, d_me),
            device_id_type=MESH,
        )

    def gather(k, carry):
        dest = dest_of(k)
        gather_rows(rows, table, picked, dest)
        pack_rows(counts, picked, packed, dest)
        return carry

    def gather_step(k, carry):
        gather(k, 0)
        dom_copy(0, k - 1).start()
        return carry

    gather(0, 0)
    lax.fori_loop(1, n_dom - 1, gather_step, 0)
    for level in range(LAYERS):
        comb[level][GROUPS + d_me] = jnp.zeros((TILE, LANES), BF)

    dom_copy(0, n_dom - 2).start()
    send_level(1)
    load_feats.wait()

    def start_group(g, carry):
        for c in range(2):
            own = [
                feats[pl.ds(pl.multiple_of((g * PACK + t) * TILE + c * 64, 64), 64), :]
                for t in range(PACK)
            ]
            h0 = lax.dot_general(
                jnp.concatenate(own, axis=1), w_wide[...], (((1,), (1,)), ((), ())),
                preferred_element_type=F32,
            )
            h0 = jnp.maximum(h0, 0.0).astype(BF)
            comb0[g, pl.ds(c * 64, 64), :] = h0
            initial[g, pl.ds(c * 64, 64), :] = h0
        return carry

    lax.fori_loop(0, GROUPS, start_group, 0)
    load_values.wait()
    load_weights.wait()

    def emit_rows(level, target):
        def one(g, carry):
            flipped = comb[level][g].astype(F32).T.astype(BF)
            for t in range(PACK):
                start = pl.multiple_of((g * PACK + t) * TILE, TILE)
                target(flipped[t * WIDTH:(t + 1) * WIDTH], start)
            return carry

        lax.fori_loop(0, GROUPS, one, 0)

    for level in range(LAYERS):
        beta = math.log(LAMBDA_DECAY / (level + 1) + 1.0)
        wait_level(level)
        if level + 2 < LAYERS:
            send_level(level + 2)

        def propagate(i, carry):
            g = lax.rem(f_me + 1 + i, GROUPS)
            lane = lane_ids(TILE)
            agg = jnp.zeros((TILE, LANES), F32)
            for t in range(PACK):
                r = g * PACK + t
                tiles = []
                for k in range(K):
                    column = columns[k, r]
                    tiles.append(comb[level][column >> 2] * masks[column & 3])
                lhs = jnp.concatenate([values[r, k] for k in range(K)], axis=1)
                out = jnp.dot(
                    lhs, jnp.concatenate(tiles, axis=0), preferred_element_type=F32
                )
                out = out + pltpu.roll(out, 64, 1)
                out = out + pltpu.roll(out, 32, 1)
                agg = jnp.where((lane >> 5) == t, out, agg)
            z = (1.0 - ALPHA) * agg + ALPHA * initial[g].astype(F32)
            zs[level, g] = z.astype(BF)
            return carry

        def send_z(i):
            feat_copy(zs.at[level], zr.at[level], z_send.at[level], z_recv.at[level], i).start()

        def step(i, carry):
            propagate(i, 0)
            send_z(i - 1)
            return carry

        propagate(0, 0)
        lax.fori_loop(1, NFEAT, step, 0)
        zr[level, f_me] = zs[level, f_me]

        def push(part, start):
            pushed[level, :, pl.ds(start, TILE)] = part

        emit_rows(level, push)

        def wait_z(i, carry):
            feat_copy(
                zs.at[level], zr.at[level], z_send.at[level], z_recv.at[level], i
            ).wait_recv()
            return carry

        lax.fori_loop(0, NFEAT - 1, wait_z, 0)

        def mix(c, carry):
            start = pl.multiple_of(c * 32, 32)
            parts = [zr[level, f, pl.ds(start, 32), :].astype(F32) for f in range(NFEAT)]
            left = swap_blocks(parts[:4])
            right = swap_blocks(parts[4:])
            block = jnp.concatenate(
                [jnp.concatenate([left[t], right[t]], axis=1) for t in range(PACK)], axis=0
            )
            product = jnp.dot(block.astype(BF), weights[level], preferred_element_type=F32)
            fresh = jnp.maximum((1.0 - beta) * block + beta * product, 0.0)
            for a in range(2):
                outs = swap_blocks(
                    [fresh[t * 32:(t + 1) * 32, a * LANES:(a + 1) * LANES] for t in range(PACK)]
                )
                for b in range(PACK):
                    hs[level, a * PACK + b, pl.ds(start, 32), :] = outs[b].astype(BF)
            return carry

        lax.fori_loop(0, 4, mix, 0)
        comb[level + 1][f_me] = hs[level, f_me]

        def send_h(i, carry):
            feat_copy(
                hs.at[level], comb[level + 1], h_send.at[level], h_recv.at[level], i
            ).start()
            return carry

        def wait_h(i, carry):
            feat_copy(
                hs.at[level], comb[level + 1], h_send.at[level], h_recv.at[level], i
            ).wait_recv()
            return carry

        lax.fori_loop(0, NFEAT - 1, send_h, 0)
        lax.fori_loop(0, NFEAT - 1, wait_h, 0)

    def finish(part, start):
        final[:, pl.ds(start, TILE)] = part

    emit_rows(LAYERS, finish)

    for level in range(LAYERS):
        def drain_dom(k, carry):
            dom_copy(level, k).wait_send()
            return carry

        def drain_feat(i, carry):
            feat_copy(
                zs.at[level], zr.at[level], z_send.at[level], z_recv.at[level], i
            ).wait_send()
            feat_copy(
                hs.at[level], comb[level + 1], h_send.at[level], h_recv.at[level], i
            ).wait_send()
            return carry

        lax.fori_loop(0, n_dom - 1, drain_dom, 0)
        lax.fori_loop(0, NFEAT - 1, drain_feat, 0)


def on_device(
    n_dom, features, w_input, layer_weights, history, tile_values, tile_columns, send_rows, send_counts
):
    grid_x, grid_z = (4, 8) if n_dom == 32 else (1, n_dom)
    table_t = history.transpose(0, 2, 1).reshape(LAYERS * WIDTH, NODES_DEV)
    vmem = pl.BlockSpec(memory_space=pltpu.VMEM)
    smem = pl.BlockSpec(memory_space=pltpu.SMEM)
    hbm = pl.BlockSpec(memory_space=pl.ANY)
    sem = pltpu.SemaphoreType.DMA
    pushed, final = pl.pallas_call(
        functools.partial(layer_kernel, n_dom, grid_x, grid_z),
        out_shape=(
            jax.ShapeDtypeStruct((LAYERS, WIDTH, NODES_DEV), BF),
            jax.ShapeDtypeStruct((WIDTH, NODES_DEV), BF),
        ),
        in_specs=[smem, smem, smem, hbm, hbm, vmem, hbm, hbm],
        out_specs=(vmem, vmem),
        scratch_shapes=[
            pltpu.VMEM((LAYERS * WIDTH, NODES_DEV), BF),
            pltpu.VMEM((NODES_DEV, LANES), F32),
            pltpu.VMEM((CAP, LANES), F32),
            pltpu.VMEM((LAYERS, n_dom, TILE, LANES), BF),
            pltpu.VMEM((PACK, TILE, LANES), BF),
            pltpu.VMEM((LANES, PACK * TILE), BF),
            *[pltpu.VMEM((GROUPS + n_dom, TILE, LANES), BF) for _ in range(LAYERS)],
            pltpu.VMEM((GROUPS, TILE, LANES), BF),
            pltpu.VMEM((GROUPS, TILE, LANES), BF),
            pltpu.VMEM((NODES_DEV, LANES), BF),
            pltpu.VMEM((NODES_DEV // TILE, K, TILE, TILE), BF),
            pltpu.VMEM((LAYERS, F, F), BF),
            pltpu.VMEM((LAYERS, NFEAT, TILE, LANES), BF),
            pltpu.VMEM((LAYERS, NFEAT, TILE, LANES), BF),
            pltpu.VMEM((LAYERS, NFEAT, TILE, LANES), BF),
            sem((4,)),
            sem((LAYERS, n_dom - 1)),
            sem((LAYERS, n_dom - 1)),
            sem((LAYERS, NFEAT - 1)),
            sem((LAYERS, NFEAT - 1)),
            sem((LAYERS, NFEAT - 1)),
            sem((LAYERS, NFEAT - 1)),
        ],
        compiler_params=pltpu.CompilerParams(collective_id=0, has_side_effects=True),
        name="halo_layers",
    )(
        tile_columns.T, send_rows.reshape(-1), send_counts, table_t, features, w_input.T,
        tile_values, layer_weights,
    )
    return pushed.transpose(0, 2, 1), final.transpose(1, 0)


def solution(mesh):
    placed = (
        P("dom", None),
        P(None, "feat"),
        P(),
        P(None, "dom", "feat"),
        P("dom", None, None, None),
        P("dom", None),
        P("dom", None, None),
        P("dom", None),
    )
    return jax.shard_map(
        functools.partial(on_device, mesh.shape["dom"]),
        mesh=mesh,
        in_specs=placed,
        out_specs=(P(None, "dom", "feat"), P("dom", "feat")),
        check_vma=False,
    )
```

```python
import functools
import math

import jax
import jax.numpy as jnp
from jax import lax
from jax.experimental import pallas as pl
from jax.experimental.pallas import tpu as pltpu
from jax.sharding import PartitionSpec as P

MESH = pl.DeviceIdType.MESH
LAYERS = 4
ALPHA = 0.1
LAMBDA_DECAY = 0.5
TILE = 128
HALF = 64
LANES = 128
PACK = 4
WIDTH = 32
NFEAT = 8
GROUPS = 8
CAP = 512
NODES_DEV = 4096
F = 256
K = 6
BF = jnp.bfloat16
F32 = jnp.float32


def lane_ids(rows):
    return lax.broadcasted_iota(jnp.int32, (rows, LANES), 1)


def swap_blocks(parts):
    x0, x1, x2, x3 = parts
    lane = lane_ids(x0.shape[0])
    low = lane < 64
    even = (lane & 32) == 0
    a0 = jnp.where(low, x0, pltpu.roll(x2, 64, 1))
    a2 = jnp.where(low, pltpu.roll(x0, 64, 1), x2)
    a1 = jnp.where(low, x1, pltpu.roll(x3, 64, 1))
    a3 = jnp.where(low, pltpu.roll(x1, 64, 1), x3)
    y0 = jnp.where(even, a0, pltpu.roll(a1, 32, 1))
    y1 = jnp.where(even, pltpu.roll(a0, 96, 1), a1)
    y2 = jnp.where(even, a2, pltpu.roll(a3, 32, 1))
    y3 = jnp.where(even, pltpu.roll(a2, 96, 1), a3)
    return y0, y1, y2, y3


def fill_table(table_t, table):
    def block(i, carry):
        start = pl.multiple_of(i * TILE, TILE)
        table[pl.ds(start, TILE), :] = table_t[:, pl.ds(start, TILE)].T.astype(F32)
        return carry

    lax.fori_loop(0, NODES_DEV // TILE, block, 0)


def gather_rows(rows, table, picked, dest):
    high, low = dest // 8, dest % 8
    for t in range(PACK):
        for i in range(TILE):
            picked[pl.ds(t * TILE + i, 1), :] = table[pl.ds(rows[high, t, low, i], 1), :]


def pack_rows(counts, picked, packed, dest):
    row = lax.broadcasted_iota(jnp.int32, (32, LANES), 0)
    count = counts[0, dest]
    for c in range(4):
        parts = []
        for t in range(PACK):
            start = t * TILE + c * 32
            live = row < count - start
            parts.append(jnp.where(live, picked[pl.ds(start, 32), :], 0.0))
        for level, part in enumerate(swap_blocks(parts)):
            packed[level, dest, pl.ds(c * 32, 32), :] = part.astype(BF)


def layer_kernel(
    n_dom, grid_x, grid_z,
    columns, rows, counts, table_hbm, feats_hbm, w_in_t, values_hbm, weights_hbm,
    pushed, final,
    table_t, table, picked, packed, masks, w_wide,
    comb0, comb1, comb2, comb3, last, initial, feats, values, weights, zs, zr, hs,
    load_sem, dom_send, dom_recv, z_send, z_recv, h_send, h_recv,
):
    comb = (comb0, comb1, comb2, comb3, last)
    f_me = lax.axis_index("feat")
    d_me = lax.axis_index("dom")
    x_me, z_me = d_me // grid_z, d_me % grid_z

    barrier = pltpu.get_barrier_semaphore()

    def greet_dom(i, carry):
        pl.semaphore_signal(
            barrier, inc=1, device_id=(f_me, lax.rem(d_me + 1 + i, n_dom)), device_id_type=MESH
        )
        return carry

    def feat_peer(i, sign):
        pair, odd = i // 2, lax.rem(i, 2)
        step = jnp.where(pair == 0, 2, jnp.where(pair == 1, 1, jnp.where(pair == 2, 3, 0)))
        flip = jnp.where(pair == 3, 1 - odd, odd)
        chip = lax.rem(f_me // 2 + 4 + sign * step, 4)
        return chip * 2 + lax.rem(f_me + flip, 2)

    def greet_feat(i, carry):
        pl.semaphore_signal(
            barrier, inc=1, device_id=(feat_peer(i, 1), d_me), device_id_type=MESH
        )
        return carry

    lax.fori_loop(0, n_dom - 1, greet_dom, 0)
    lax.fori_loop(0, NFEAT - 1, greet_feat, 0)
    load_table = pltpu.make_async_copy(table_hbm, table_t, load_sem.at[0])
    load_feats = pltpu.make_async_copy(feats_hbm, feats, load_sem.at[1])
    load_values = pltpu.make_async_copy(values_hbm, values, load_sem.at[2])
    load_weights = pltpu.make_async_copy(weights_hbm, weights, load_sem.at[3])
    load_table.start()
    load_feats.start()
    load_values.start()
    load_weights.start()
    lane = lane_ids(TILE)
    for b in range(PACK):
        masks[b] = jnp.where((lane >> 5) == b, 1.0, 0.0).astype(BF)
    w_wide[...] = jnp.zeros((LANES, PACK * TILE), BF)
    for t in range(PACK):
        w_wide[t * WIDTH:(t + 1) * WIDTH, t * TILE:(t + 1) * TILE] = w_in_t[...]
    load_table.wait()
    fill_table(table_t, table)
    pl.semaphore_wait(barrier, n_dom - 1 + NFEAT - 1)

    def dest_of(k):
        i = lax.rem(k, grid_z)
        half = grid_z // 2
        dz = jnp.where(lax.rem(i, 2) == 1, half - (i + 1) // 2, half + i // 2)
        dx = lax.rem(grid_x - 1 - k // grid_z + i + 1, grid_x)
        return lax.rem(x_me + dx, grid_x) * grid_z + lax.rem(z_me + dz, grid_z)

    def dom_copy(level, k):
        dest = dest_of(k)
        return pltpu.make_async_remote_copy(
            src_ref=packed.at[level, dest],
            dst_ref=comb[level].at[GROUPS + d_me],
            send_sem=dom_send.at[level, k],
            recv_sem=dom_recv.at[level, k],
            device_id=(f_me, dest),
            device_id_type=MESH,
        )

    def send_level(level):
        def one(k, carry):
            dom_copy(level, k).start()
            return carry

        lax.fori_loop(0, n_dom - 1, one, 0)

    def wait_level(level):
        def one(k, carry):
            dom_copy(level, k).wait_recv()
            return carry

        lax.fori_loop(0, n_dom - 1, one, 0)

    def z_copy(level, i):
        dest = feat_peer(i, 1)
        return pltpu.make_async_remote_copy(
            src_ref=zs.at[level, dest],
            dst_ref=zr.at[level, f_me],
            send_sem=z_send.at[level, i],
            recv_sem=z_recv.at[level, i],
            device_id=(dest, d_me),
            device_id_type=MESH,
        )

    def h_copy(level, half, i):
        dest = feat_peer(i, 1)
        part = pl.ds(pl.multiple_of(half * HALF, HALF), HALF)
        return pltpu.make_async_remote_copy(
            src_ref=hs.at[level, dest, part],
            dst_ref=comb[level + 1].at[f_me, part],
            send_sem=h_send.at[level, half, i],
            recv_sem=h_recv.at[level, half, i],
            device_id=(dest, d_me),
            device_id_type=MESH,
        )

    def gather(k, carry):
        dest = dest_of(k)
        gather_rows(rows, table, picked, dest)
        pack_rows(counts, picked, packed, dest)
        return carry

    def gather_step(k, carry):
        gather(k, 0)
        dom_copy(0, k - 1).start()
        return carry

    gather(0, 0)
    lax.fori_loop(1, n_dom - 1, gather_step, 0)
    for level in range(LAYERS):
        comb[level][GROUPS + d_me] = jnp.zeros((TILE, LANES), BF)

    dom_copy(0, n_dom - 2).start()
    send_level(1)
    load_feats.wait()

    def start_group(g, carry):
        for c in range(2):
            own = [
                feats[pl.ds(pl.multiple_of((g * PACK + t) * TILE + c * 64, 64), 64), :]
                for t in range(PACK)
            ]
            h0 = lax.dot_general(
                jnp.concatenate(own, axis=1), w_wide[...], (((1,), (1,)), ((), ())),
                preferred_element_type=F32,
            )
            h0 = jnp.maximum(h0, 0.0).astype(BF)
            comb0[g, pl.ds(c * 64, 64), :] = h0
            initial[g, pl.ds(c * 64, 64), :] = h0
        return carry

    lax.fori_loop(0, GROUPS, start_group, 0)
    load_values.wait()
    load_weights.wait()

    def emit_group(level, g, target):
        flipped = comb[level][g].T
        for t in range(PACK):
            start = pl.multiple_of((g * PACK + t) * TILE, TILE)
            target(flipped[t * WIDTH:(t + 1) * WIDTH], start)

    for level in range(LAYERS):
        beta = math.log(LAMBDA_DECAY / (level + 1) + 1.0)
        wait_level(level)
        if level + 2 < LAYERS:
            send_level(level + 2)

        def propagate(i, carry):
            g = feat_peer(i, 1)
            lane = lane_ids(TILE)
            agg = jnp.zeros((TILE, LANES), F32)
            for t in range(PACK):
                r = g * PACK + t
                tiles = []
                for k in range(K):
                    column = columns[k, r]
                    tiles.append(comb[level][column >> 2] * masks[column & 3])
                lhs = jnp.concatenate([values[r, k] for k in range(K)], axis=1)
                out = jnp.dot(
                    lhs, jnp.concatenate(tiles, axis=0), preferred_element_type=F32
                )
                out = out + pltpu.roll(out, 64, 1)
                out = out + pltpu.roll(out, 32, 1)
                agg = jnp.where((lane >> 5) == t, out, agg)
            z = (1.0 - ALPHA) * agg + ALPHA * initial[g].astype(F32)
            zs[level, g] = z.astype(BF)
            return carry

        def step(i, carry):
            propagate(i, 0)
            z_copy(level, i - 1).start()
            return carry

        propagate(0, 0)
        lax.fori_loop(1, NFEAT, step, 0)
        zr[level, f_me] = zs[level, f_me]

        def push(part, start):
            pushed[level, :, pl.ds(start, TILE)] = part

        def push_group(g, carry):
            emit_group(level, g, push)
            return carry

        lax.fori_loop(0, GROUPS, push_group, 0)

        def wait_z(i, carry):
            z_copy(level, i).wait_recv()
            return carry

        lax.fori_loop(0, NFEAT - 1, wait_z, 0)

        def mix(half, piece):
            start = pl.multiple_of(half * HALF + piece * 32, 32)
            parts = [zr[level, f, pl.ds(start, 32), :].astype(F32) for f in range(NFEAT)]
            left = swap_blocks(parts[:4])
            right = swap_blocks(parts[4:])
            block = jnp.concatenate(
                [jnp.concatenate([left[t], right[t]], axis=1) for t in range(PACK)], axis=0
            )
            product = jnp.dot(block.astype(BF), weights[level], preferred_element_type=F32)
            fresh = jnp.maximum((1.0 - beta) * block + beta * product, 0.0)
            for a in range(2):
                outs = swap_blocks(
                    [fresh[t * 32:(t + 1) * 32, a * LANES:(a + 1) * LANES] for t in range(PACK)]
                )
                for b in range(PACK):
                    hs[level, a * PACK + b, pl.ds(start, 32), :] = outs[b].astype(BF)

        def mix_half(half, carry):
            mix(half, 0)
            mix(half, 1)

            def send_h(i, inner):
                h_copy(level, half, i).start()
                return inner

            lax.fori_loop(0, NFEAT - 1, send_h, 0)
            return carry

        lax.fori_loop(0, 2, mix_half, 0)
        comb[level + 1][f_me] = hs[level, f_me]

        def wait_h(i, carry):
            h_copy(level, 0, i).wait_recv()
            h_copy(level, 1, i).wait_recv()
            return carry

        if level + 1 < LAYERS:
            lax.fori_loop(0, NFEAT - 1, wait_h, 0)

    def finish(part, start):
        final[:, pl.ds(start, TILE)] = part

    def finish_group(i, carry):
        wait_h(i, 0)
        emit_group(LAYERS, feat_peer(i, -1), finish)
        return carry

    emit_group(LAYERS, f_me, finish)
    lax.fori_loop(0, NFEAT - 1, finish_group, 0)

    for level in range(LAYERS):
        def drain_dom(k, carry):
            dom_copy(level, k).wait_send()
            return carry

        def drain_feat(i, carry):
            z_copy(level, i).wait_send()
            h_copy(level, 0, i).wait_send()
            h_copy(level, 1, i).wait_send()
            return carry

        lax.fori_loop(0, n_dom - 1, drain_dom, 0)
        lax.fori_loop(0, NFEAT - 1, drain_feat, 0)


def on_device(
    n_dom, features, w_input, layer_weights, history, tile_values, tile_columns, send_rows, send_counts
):
    grid_x, grid_z = (4, 8) if n_dom == 32 else (1, n_dom)
    table_t = history.transpose(0, 2, 1).reshape(LAYERS * WIDTH, NODES_DEV)
    vmem = pl.BlockSpec(memory_space=pltpu.VMEM)
    smem = pl.BlockSpec(memory_space=pltpu.SMEM)
    hbm = pl.BlockSpec(memory_space=pl.ANY)
    sem = pltpu.SemaphoreType.DMA
    pushed, final = pl.pallas_call(
        functools.partial(layer_kernel, n_dom, grid_x, grid_z),
        out_shape=(
            pltpu.VMEM((LAYERS, WIDTH, NODES_DEV), BF),
            pltpu.VMEM((WIDTH, NODES_DEV), BF),
        ),
        in_specs=[smem, smem, smem, hbm, hbm, vmem, hbm, hbm],
        out_specs=(vmem, vmem),
        scratch_shapes=[
            pltpu.VMEM((LAYERS * WIDTH, NODES_DEV), BF),
            pltpu.VMEM((NODES_DEV, LANES), F32),
            pltpu.VMEM((CAP, LANES), F32),
            pltpu.VMEM((LAYERS, n_dom, TILE, LANES), BF),
            pltpu.VMEM((PACK, TILE, LANES), BF),
            pltpu.VMEM((LANES, PACK * TILE), BF),
            *[pltpu.VMEM((GROUPS + n_dom, TILE, LANES), BF) for _ in range(LAYERS)],
            pltpu.VMEM((GROUPS, TILE, LANES), BF),
            pltpu.VMEM((GROUPS, TILE, LANES), BF),
            pltpu.VMEM((NODES_DEV, LANES), BF),
            pltpu.VMEM((NODES_DEV // TILE, K, TILE, TILE), BF),
            pltpu.VMEM((LAYERS, F, F), BF),
            pltpu.VMEM((LAYERS, NFEAT, TILE, LANES), BF),
            pltpu.VMEM((LAYERS, NFEAT, TILE, LANES), BF),
            pltpu.VMEM((LAYERS, NFEAT, TILE, LANES), BF),
            sem((4,)),
            sem((LAYERS, n_dom - 1)),
            sem((LAYERS, n_dom - 1)),
            sem((LAYERS, NFEAT - 1)),
            sem((LAYERS, NFEAT - 1)),
            sem((LAYERS, 2, NFEAT - 1)),
            sem((LAYERS, 2, NFEAT - 1)),
        ],
        compiler_params=pltpu.CompilerParams(collective_id=0, has_side_effects=True),
        name="halo_layers",
    )(
        tile_columns.T, send_rows.reshape(n_dom // 8, 8, PACK, TILE).transpose(0, 2, 1, 3), send_counts, table_t, features, w_input.T,
        tile_values, layer_weights,
    )
    return pushed.transpose(0, 2, 1), final.transpose(1, 0)


def solution(mesh):
    placed = (
        P("dom", None),
        P(None, "feat"),
        P(),
        P(None, "dom", "feat"),
        P("dom", None, None, None),
        P("dom", None),
        P("dom", None, None),
        P("dom", None),
    )
    return jax.shard_map(
        functools.partial(on_device, mesh.shape["dom"]),
        mesh=mesh,
        in_specs=placed,
        out_specs=(P(None, "dom", "feat"), P("dom", "feat")),
        check_vma=False,
    )
```

```python
import functools
import math

import jax
import jax.numpy as jnp
from jax import lax
from jax.experimental import pallas as pl
from jax.experimental.pallas import tpu as pltpu
from jax.sharding import PartitionSpec as P

MESH = pl.DeviceIdType.MESH
LAYERS = 4
ALPHA = 0.1
LAMBDA_DECAY = 0.5
TILE = 128
HALF = 64
LANES = 128
PACK = 4
WIDTH = 32
NFEAT = 8
GROUPS = 8
CAP = 512
NODES_DEV = 4096
F = 256
K = 6
BF = jnp.bfloat16
F32 = jnp.float32


def lane_ids(rows):
    return lax.broadcasted_iota(jnp.int32, (rows, LANES), 1)


def swap_blocks(parts):
    x0, x1, x2, x3 = parts
    lane = lane_ids(x0.shape[0])
    low = lane < 64
    even = (lane & 32) == 0
    a0 = jnp.where(low, x0, pltpu.roll(x2, 64, 1))
    a2 = jnp.where(low, pltpu.roll(x0, 64, 1), x2)
    a1 = jnp.where(low, x1, pltpu.roll(x3, 64, 1))
    a3 = jnp.where(low, pltpu.roll(x1, 64, 1), x3)
    y0 = jnp.where(even, a0, pltpu.roll(a1, 32, 1))
    y1 = jnp.where(even, pltpu.roll(a0, 96, 1), a1)
    y2 = jnp.where(even, a2, pltpu.roll(a3, 32, 1))
    y3 = jnp.where(even, pltpu.roll(a2, 96, 1), a3)
    return y0, y1, y2, y3


def fill_table(table_t, table, piece):
    def block(i, carry):
        for u in range(4):
            start = pl.multiple_of((piece * 8 + i * 4 + u) * TILE, TILE)
            table[pl.ds(start, TILE), :] = table_t[:, pl.ds(start, TILE)].T.astype(F32)
        return carry

    lax.fori_loop(0, 2, block, 0)


def gather_rows(rows, table, picked, dest):
    high, low = dest // 8, dest % 8
    for t in range(PACK):
        for i in range(TILE):
            picked[pl.ds(t * TILE + i, 1), :] = table[pl.ds(rows[high, t, low, i], 1), :]


def pack_rows(counts, picked, packed, dest):
    row = lax.broadcasted_iota(jnp.int32, (32, LANES), 0)
    count = counts[0, dest]
    for c in range(4):
        parts = []
        for t in range(PACK):
            start = t * TILE + c * 32
            live = row < count - start
            parts.append(jnp.where(live, picked[pl.ds(start, 32), :], 0.0))
        for level, part in enumerate(swap_blocks(parts)):
            packed[level, dest, pl.ds(c * 32, 32), :] = part.astype(BF)


def layer_kernel(
    n_dom, grid_x, grid_z,
    columns, rows, counts, table_hbm, feats_hbm, w_in_t, values_hbm, weights_hbm,
    pushed, final,
    table_t, table, picked, packed, masks, w_wide,
    comb0, comb1, comb2, comb3, last, initial, feats, values, weights, zs, zr, hs,
    table_sem, load_sem, dom_send, dom_recv, z_send, z_recv, h_send, h_recv,
):
    comb = (comb0, comb1, comb2, comb3, last)
    f_me = lax.axis_index("feat")
    d_me = lax.axis_index("dom")
    x_me, z_me = d_me // grid_z, d_me % grid_z

    def load_table(piece):
        part = pl.ds(piece * (NODES_DEV // 4), NODES_DEV // 4)
        return pltpu.make_async_copy(
            table_hbm.at[:, part], table_t.at[:, part], table_sem.at[piece]
        )

    for piece in range(4):
        load_table(piece).start()

    barrier = pltpu.get_barrier_semaphore()

    def greet_dom(i, carry):
        pl.semaphore_signal(
            barrier, inc=1, device_id=(f_me, lax.rem(d_me + 1 + i, n_dom)), device_id_type=MESH
        )
        return carry

    def feat_peer(i, sign):
        pair, odd = i // 2, lax.rem(i, 2)
        step = jnp.where(pair == 0, 2, jnp.where(pair == 1, 1, jnp.where(pair == 2, 3, 0)))
        flip = jnp.where(pair == 3, 1 - odd, odd)
        chip = lax.rem(f_me // 2 + 4 + sign * step, 4)
        return chip * 2 + lax.rem(f_me + flip, 2)

    def greet_feat(i, carry):
        pl.semaphore_signal(
            barrier, inc=1, device_id=(feat_peer(i, 1), d_me), device_id_type=MESH
        )
        return carry

    lax.fori_loop(0, n_dom - 1, greet_dom, 0)
    lax.fori_loop(0, NFEAT - 1, greet_feat, 0)
    load_feats = pltpu.make_async_copy(feats_hbm, feats, load_sem.at[1])
    load_values = pltpu.make_async_copy(values_hbm, values, load_sem.at[2])
    load_weights = pltpu.make_async_copy(weights_hbm, weights, load_sem.at[3])
    load_feats.start()
    load_values.start()
    load_weights.start()
    lane = lane_ids(TILE)
    for b in range(PACK):
        masks[b] = jnp.where((lane >> 5) == b, 1.0, 0.0).astype(BF)
    w_wide[...] = jnp.zeros((LANES, PACK * TILE), BF)
    for t in range(PACK):
        w_wide[t * WIDTH:(t + 1) * WIDTH, t * TILE:(t + 1) * TILE] = w_in_t[...]
    for piece in range(4):
        load_table(piece).wait()
        fill_table(table_t, table, piece)

    def dest_of(k):
        i = lax.rem(k, grid_z)
        half = grid_z // 2
        dz = jnp.where(lax.rem(i, 2) == 1, half - (i + 1) // 2, half + i // 2)
        dx = lax.rem(grid_x - 1 - k // grid_z + i + 1, grid_x)
        return lax.rem(x_me + dx, grid_x) * grid_z + lax.rem(z_me + dz, grid_z)

    def dom_copy(level, k):
        dest = dest_of(k)
        return pltpu.make_async_remote_copy(
            src_ref=packed.at[level, dest],
            dst_ref=comb[level].at[GROUPS + d_me],
            send_sem=dom_send.at[level, k],
            recv_sem=dom_recv.at[level, k],
            device_id=(f_me, dest),
            device_id_type=MESH,
        )

    def send_level(level):
        def one(k, carry):
            dom_copy(level, k).start()
            return carry

        lax.fori_loop(0, n_dom - 1, one, 0)

    def wait_level(level):
        def one(k, carry):
            dom_copy(level, k).wait_recv()
            return carry

        lax.fori_loop(0, n_dom - 1, one, 0)

    def z_copy(level, i):
        dest = feat_peer(i, 1)
        return pltpu.make_async_remote_copy(
            src_ref=zs.at[level, dest],
            dst_ref=zr.at[level, f_me],
            send_sem=z_send.at[level, i],
            recv_sem=z_recv.at[level, i],
            device_id=(dest, d_me),
            device_id_type=MESH,
        )

    def h_copy(level, half, i):
        dest = feat_peer(i, 1)
        part = pl.ds(pl.multiple_of(half * HALF, HALF), HALF)
        return pltpu.make_async_remote_copy(
            src_ref=hs.at[level, dest, part],
            dst_ref=comb[level + 1].at[f_me, part],
            send_sem=h_send.at[level, half, i],
            recv_sem=h_recv.at[level, half, i],
            device_id=(dest, d_me),
            device_id_type=MESH,
        )

    def gather(k, carry):
        dest = dest_of(k)
        gather_rows(rows, table, picked, dest)
        pack_rows(counts, picked, packed, dest)
        return carry

    def gather_step(k, carry):
        gather(k, 0)
        dom_copy(0, k - 1).start()
        return carry

    def send_first(k, carry):
        dom_copy(0, k).start()
        return carry

    ahead = min(2, n_dom - 1)
    lax.fori_loop(0, ahead, gather, 0)
    pl.semaphore_wait(barrier, n_dom - 1 + NFEAT - 1)
    lax.fori_loop(0, ahead - 1, send_first, 0)
    lax.fori_loop(ahead, n_dom - 1, gather_step, 0)
    for level in range(LAYERS):
        comb[level][GROUPS + d_me] = jnp.zeros((TILE, LANES), BF)

    dom_copy(0, n_dom - 2).start()
    send_level(1)
    load_feats.wait()

    def start_group(g, carry):
        for c in range(2):
            own = [
                feats[pl.ds(pl.multiple_of((g * PACK + t) * TILE + c * 64, 64), 64), :]
                for t in range(PACK)
            ]
            h0 = lax.dot_general(
                jnp.concatenate(own, axis=1), w_wide[...], (((1,), (1,)), ((), ())),
                preferred_element_type=F32,
            )
            h0 = jnp.maximum(h0, 0.0).astype(BF)
            comb0[g, pl.ds(c * 64, 64), :] = h0
            initial[g, pl.ds(c * 64, 64), :] = h0
        return carry

    lax.fori_loop(0, GROUPS, start_group, 0)
    load_values.wait()
    load_weights.wait()

    def emit_group(level, g, target):
        flipped = comb[level][g].T
        for t in range(PACK):
            start = pl.multiple_of((g * PACK + t) * TILE, TILE)
            target(flipped[t * WIDTH:(t + 1) * WIDTH], start)

    def drain_h(level, i, carry):
        h_copy(level, 0, i).wait_send()
        h_copy(level, 1, i).wait_send()
        return carry

    for level in range(LAYERS):
        beta = math.log(LAMBDA_DECAY / (level + 1) + 1.0)
        wait_level(level)
        if level + 2 < LAYERS:
            send_level(level + 2)

        def propagate(i, carry):
            g = feat_peer(i, 1)
            lane = lane_ids(TILE)
            agg = jnp.zeros((TILE, LANES), F32)
            for t in range(PACK):
                r = g * PACK + t
                tiles = []
                for k in range(K):
                    column = columns[k, r]
                    tiles.append(comb[level][column >> 2] * masks[column & 3])
                lhs = jnp.concatenate([values[r, k] for k in range(K)], axis=1)
                out = jnp.dot(
                    lhs, jnp.concatenate(tiles, axis=0), preferred_element_type=F32
                )
                out = out + pltpu.roll(out, 64, 1)
                out = out + pltpu.roll(out, 32, 1)
                agg = jnp.where((lane >> 5) == t, out, agg)
            z = (1.0 - ALPHA) * agg + ALPHA * initial[g].astype(F32)
            zs[level, g] = z.astype(BF)
            return carry

        def step(i, carry):
            propagate(i, 0)
            z_copy(level, i - 1).start()
            return carry

        propagate(0, 0)
        lax.fori_loop(1, NFEAT, step, 0)
        zr[level, f_me] = zs[level, f_me]

        def push(part, start):
            pushed[level, :, pl.ds(start, TILE)] = part

        def push_group(g, carry):
            emit_group(level, g, push)
            return carry

        lax.fori_loop(0, GROUPS, push_group, 0)

        def wait_z(i, carry):
            z_copy(level, i).wait_recv()
            return carry

        lax.fori_loop(0, NFEAT - 1, wait_z, 0)

        def mix(half, piece):
            start = pl.multiple_of(half * HALF + piece * 32, 32)
            parts = [zr[level, f, pl.ds(start, 32), :].astype(F32) for f in range(NFEAT)]
            left = swap_blocks(parts[:4])
            right = swap_blocks(parts[4:])
            block = jnp.concatenate(
                [jnp.concatenate([left[t], right[t]], axis=1) for t in range(PACK)], axis=0
            )
            product = jnp.dot(block.astype(BF), weights[level], preferred_element_type=F32)
            fresh = jnp.maximum((1.0 - beta) * block + beta * product, 0.0)
            for a in range(2):
                outs = swap_blocks(
                    [fresh[t * 32:(t + 1) * 32, a * LANES:(a + 1) * LANES] for t in range(PACK)]
                )
                for b in range(PACK):
                    hs[level, a * PACK + b, pl.ds(start, 32), :] = outs[b].astype(BF)

        def mix_half(half, carry):
            mix(half, 0)
            mix(half, 1)

            def send_h(i, inner):
                h_copy(level, half, i).start()
                return inner

            lax.fori_loop(0, NFEAT - 1, send_h, 0)
            return carry

        lax.fori_loop(0, 2, mix_half, 0)
        comb[level + 1][f_me] = hs[level, f_me]

        def drain_dom(k, carry):
            dom_copy(level, k).wait_send()
            return carry

        def drain_z(i, carry):
            z_copy(level, i).wait_send()
            return carry

        lax.fori_loop(0, n_dom - 1, drain_dom, 0)
        lax.fori_loop(0, NFEAT - 1, drain_z, 0)
        if level > 0:
            lax.fori_loop(0, NFEAT - 1, functools.partial(drain_h, level - 1), 0)

        def wait_h(i, carry):
            h_copy(level, 0, i).wait_recv()
            h_copy(level, 1, i).wait_recv()
            return carry

        if level + 1 < LAYERS:
            lax.fori_loop(0, NFEAT - 1, wait_h, 0)

    def finish(part, start):
        final[:, pl.ds(start, TILE)] = part

    def finish_group(i, carry):
        wait_h(i, 0)
        emit_group(LAYERS, feat_peer(i, -1), finish)
        return carry

    emit_group(LAYERS, f_me, finish)
    lax.fori_loop(0, NFEAT - 1, finish_group, 0)

    lax.fori_loop(0, NFEAT - 1, functools.partial(drain_h, LAYERS - 1), 0)


def on_device(
    n_dom, features, w_input, layer_weights, history, tile_values, tile_columns, send_rows, send_counts
):
    grid_x, grid_z = (4, 8) if n_dom == 32 else (1, n_dom)
    table_t = history.transpose(0, 2, 1).reshape(LAYERS * WIDTH, NODES_DEV)
    vmem = pl.BlockSpec(memory_space=pltpu.VMEM)
    smem = pl.BlockSpec(memory_space=pltpu.SMEM)
    hbm = pl.BlockSpec(memory_space=pl.ANY)
    sem = pltpu.SemaphoreType.DMA
    pushed, final = pl.pallas_call(
        functools.partial(layer_kernel, n_dom, grid_x, grid_z),
        out_shape=(
            pltpu.VMEM((LAYERS, WIDTH, NODES_DEV), BF),
            pltpu.VMEM((WIDTH, NODES_DEV), BF),
        ),
        in_specs=[smem, smem, smem, hbm, hbm, vmem, hbm, hbm],
        out_specs=(vmem, vmem),
        scratch_shapes=[
            pltpu.VMEM((LAYERS * WIDTH, NODES_DEV), BF),
            pltpu.VMEM((NODES_DEV, LANES), F32),
            pltpu.VMEM((CAP, LANES), F32),
            pltpu.VMEM((LAYERS, n_dom, TILE, LANES), BF),
            pltpu.VMEM((PACK, TILE, LANES), BF),
            pltpu.VMEM((LANES, PACK * TILE), BF),
            *[pltpu.VMEM((GROUPS + n_dom, TILE, LANES), BF) for _ in range(LAYERS)],
            pltpu.VMEM((GROUPS, TILE, LANES), BF),
            pltpu.VMEM((GROUPS, TILE, LANES), BF),
            pltpu.VMEM((NODES_DEV, LANES), BF),
            pltpu.VMEM((NODES_DEV // TILE, K, TILE, TILE), BF),
            pltpu.VMEM((LAYERS, F, F), BF),
            pltpu.VMEM((LAYERS, NFEAT, TILE, LANES), BF),
            pltpu.VMEM((LAYERS, NFEAT, TILE, LANES), BF),
            pltpu.VMEM((LAYERS, NFEAT, TILE, LANES), BF),
            sem((4,)),
            sem((4,)),
            sem((LAYERS, n_dom - 1)),
            sem((LAYERS, n_dom - 1)),
            sem((LAYERS, NFEAT - 1)),
            sem((LAYERS, NFEAT - 1)),
            sem((LAYERS, 2, NFEAT - 1)),
            sem((LAYERS, 2, NFEAT - 1)),
        ],
        compiler_params=pltpu.CompilerParams(collective_id=0, has_side_effects=True),
        name="halo_layers",
    )(
        tile_columns.T, send_rows.reshape(n_dom // 8, 8, PACK, TILE).transpose(0, 2, 1, 3), send_counts, table_t, features, w_input.T,
        tile_values, layer_weights,
    )
    return pushed.transpose(0, 2, 1), final.transpose(1, 0)


def solution(mesh):
    placed = (
        P("dom", None),
        P(None, "feat"),
        P(),
        P(None, "dom", "feat"),
        P("dom", None, None, None),
        P("dom", None),
        P("dom", None, None),
        P("dom", None),
    )
    return jax.shard_map(
        functools.partial(on_device, mesh.shape["dom"]),
        mesh=mesh,
        in_specs=placed,
        out_specs=(P(None, "dom", "feat"), P("dom", "feat")),
        check_vma=False,
    )
```

```python
import functools
import math

import jax
import jax.numpy as jnp
from jax import lax
from jax.experimental import pallas as pl
from jax.experimental.pallas import tpu as pltpu
from jax.sharding import PartitionSpec as P

MESH = pl.DeviceIdType.MESH
LAYERS = 4
ALPHA = 0.1
LAMBDA_DECAY = 0.5
TILE = 128
HALF = 64
LANES = 128
PACK = 4
WIDTH = 32
NFEAT = 8
GROUPS = 8
CAP = 512
NODES_DEV = 4096
F = 256
K = 6
BF = jnp.bfloat16
F32 = jnp.float32


def lane_ids(rows):
    return lax.broadcasted_iota(jnp.int32, (rows, LANES), 1)


def swap_blocks(parts):
    x0, x1, x2, x3 = parts
    lane = lane_ids(x0.shape[0])
    low = lane < 64
    even = (lane & 32) == 0
    a0 = jnp.where(low, x0, pltpu.roll(x2, 64, 1))
    a2 = jnp.where(low, pltpu.roll(x0, 64, 1), x2)
    a1 = jnp.where(low, x1, pltpu.roll(x3, 64, 1))
    a3 = jnp.where(low, pltpu.roll(x1, 64, 1), x3)
    y0 = jnp.where(even, a0, pltpu.roll(a1, 32, 1))
    y1 = jnp.where(even, pltpu.roll(a0, 96, 1), a1)
    y2 = jnp.where(even, a2, pltpu.roll(a3, 32, 1))
    y3 = jnp.where(even, pltpu.roll(a2, 96, 1), a3)
    return y0, y1, y2, y3


def fill_table(table_t, table, piece):
    def block(i, carry):
        for u in range(4):
            start = pl.multiple_of((piece * 8 + i * 4 + u) * TILE, TILE)
            table[pl.ds(start, TILE), :] = table_t[:, pl.ds(start, TILE)].T.astype(F32)
        return carry

    lax.fori_loop(0, 2, block, 0)


def gather_rows(rows, table, picked, dest):
    high, low = dest // 8, dest % 8
    for t in range(PACK):
        for i in range(TILE):
            picked[pl.ds(t * TILE + i, 1), :] = table[pl.ds(rows[high, t, low, i], 1), :]


def pack_rows(counts, picked, packed, dest):
    row = lax.broadcasted_iota(jnp.int32, (32, LANES), 0)
    count = counts[0, dest]
    for c in range(4):
        parts = []
        for t in range(PACK):
            start = t * TILE + c * 32
            live = row < count - start
            parts.append(jnp.where(live, picked[pl.ds(start, 32), :], 0.0))
        for level, part in enumerate(swap_blocks(parts)):
            packed[level, dest, pl.ds(c * 32, 32), :] = part.astype(BF)


def layer_kernel(
    n_dom, grid_x, grid_z,
    columns, rows, counts, table_hbm, feats_hbm, w_in_t, values_hbm, weights_hbm,
    pushed, final,
    table_t, table, picked, packed, masks, w_wide,
    comb0, comb1, comb2, comb3, last, initial, feats, values, weights, zs, zr, hs,
    table_sem, load_sem, dom_send, dom_recv, z_send, z_recv, h_send, h_recv,
):
    comb = (comb0, comb1, comb2, comb3, last)
    f_me = lax.axis_index("feat")
    d_me = lax.axis_index("dom")
    x_me, z_me = d_me // grid_z, d_me % grid_z

    def load_table(piece):
        part = pl.ds(piece * (NODES_DEV // 4), NODES_DEV // 4)
        return pltpu.make_async_copy(
            table_hbm.at[:, part], table_t.at[:, part], table_sem.at[piece]
        )

    for piece in range(4):
        load_table(piece).start()

    barrier = pltpu.get_barrier_semaphore()

    def dest_of(k):
        i = lax.rem(k, grid_z)
        half = grid_z // 2
        dz = jnp.where(lax.rem(i, 2) == 1, half - (i + 1) // 2, half + i // 2)
        dx = lax.rem(grid_x - 1 - k // grid_z + i + 1, grid_x)
        return lax.rem(x_me + dx, grid_x) * grid_z + lax.rem(z_me + dz, grid_z)

    def greet_dom(i, carry):
        pl.semaphore_signal(
            barrier, inc=1, device_id=(f_me, dest_of(i)), device_id_type=MESH
        )
        return carry

    def feat_peer(i, sign):
        pair, odd = i // 2, lax.rem(i, 2)
        step = jnp.where(pair == 0, 2, jnp.where(pair == 1, 1, jnp.where(pair == 2, 3, 0)))
        flip = jnp.where(pair == 3, 1 - odd, odd)
        chip = lax.rem(f_me // 2 + 4 + sign * step, 4)
        return chip * 2 + lax.rem(f_me + flip, 2)

    def greet_feat(i, carry):
        pl.semaphore_signal(
            barrier, inc=1, device_id=(feat_peer(i, 1), d_me), device_id_type=MESH
        )
        return carry

    lax.fori_loop(0, n_dom - 1, greet_dom, 0)
    lax.fori_loop(0, NFEAT - 1, greet_feat, 0)
    load_feats = pltpu.make_async_copy(feats_hbm, feats, load_sem.at[1])
    load_values = pltpu.make_async_copy(values_hbm, values, load_sem.at[2])
    load_weights = pltpu.make_async_copy(weights_hbm, weights, load_sem.at[3])
    load_feats.start()
    load_values.start()
    load_weights.start()
    lane = lane_ids(TILE)
    for b in range(PACK):
        masks[b] = jnp.where((lane >> 5) == b, 1.0, 0.0).astype(BF)
    w_wide[...] = jnp.zeros((LANES, PACK * TILE), BF)
    for t in range(PACK):
        w_wide[t * WIDTH:(t + 1) * WIDTH, t * TILE:(t + 1) * TILE] = w_in_t[...]
    for piece in range(4):
        load_table(piece).wait()
        fill_table(table_t, table, piece)

    def dom_copy(level, k):
        dest = dest_of(k)
        return pltpu.make_async_remote_copy(
            src_ref=packed.at[level, dest],
            dst_ref=comb[level].at[GROUPS + d_me],
            send_sem=dom_send.at[level, k],
            recv_sem=dom_recv.at[level, k],
            device_id=(f_me, dest),
            device_id_type=MESH,
        )

    def send_level(level):
        def one(k, carry):
            dom_copy(level, k).start()
            return carry

        lax.fori_loop(0, n_dom - 1, one, 0)

    def wait_level(level):
        def one(k, carry):
            dom_copy(level, k).wait_recv()
            return carry

        lax.fori_loop(0, n_dom - 1, one, 0)

    def z_copy(level, i):
        dest = feat_peer(i, 1)
        return pltpu.make_async_remote_copy(
            src_ref=zs.at[level, dest],
            dst_ref=zr.at[level, f_me],
            send_sem=z_send.at[level, i],
            recv_sem=z_recv.at[level, i],
            device_id=(dest, d_me),
            device_id_type=MESH,
        )

    def h_copy(level, half, i):
        dest = feat_peer(i, 1)
        part = pl.ds(pl.multiple_of(half * HALF, HALF), HALF)
        return pltpu.make_async_remote_copy(
            src_ref=hs.at[level, dest, part],
            dst_ref=comb[level + 1].at[f_me, part],
            send_sem=h_send.at[level, half, i],
            recv_sem=h_recv.at[level, half, i],
            device_id=(dest, d_me),
            device_id_type=MESH,
        )

    def gather(k, carry):
        dest = dest_of(k)
        gather_rows(rows, table, picked, dest)
        pack_rows(counts, picked, packed, dest)
        return carry

    def gather_step(k, carry):
        gather(k, 0)
        dom_copy(0, k - 1).start()
        return carry

    def send_first(k, carry):
        dom_copy(0, k).start()
        return carry

    ahead = min(2, n_dom - 1)
    lax.fori_loop(0, ahead, gather, 0)
    pl.semaphore_wait(barrier, n_dom - 1 + NFEAT - 1)
    lax.fori_loop(0, ahead - 1, send_first, 0)
    lax.fori_loop(ahead, n_dom - 1, gather_step, 0)
    for level in range(LAYERS):
        comb[level][GROUPS + d_me] = jnp.zeros((TILE, LANES), BF)

    dom_copy(0, n_dom - 2).start()
    send_level(1)
    load_feats.wait()

    def start_group(g, carry):
        for c in range(2):
            own = [
                feats[pl.ds(pl.multiple_of((g * PACK + t) * TILE + c * 64, 64), 64), :]
                for t in range(PACK)
            ]
            h0 = lax.dot_general(
                jnp.concatenate(own, axis=1), w_wide[...], (((1,), (1,)), ((), ())),
                preferred_element_type=F32,
            )
            h0 = jnp.maximum(h0, 0.0).astype(BF)
            comb0[g, pl.ds(c * 64, 64), :] = h0
            initial[g, pl.ds(c * 64, 64), :] = h0
        return carry

    lax.fori_loop(0, GROUPS, start_group, 0)
    load_values.wait()
    load_weights.wait()

    def emit_group(level, g, target):
        flipped = comb[level][g].T
        for t in range(PACK):
            start = pl.multiple_of((g * PACK + t) * TILE, TILE)
            target(flipped[t * WIDTH:(t + 1) * WIDTH], start)

    def drain_h(level, i, carry):
        h_copy(level, 0, i).wait_send()
        h_copy(level, 1, i).wait_send()
        return carry

    for level in range(LAYERS):
        beta = math.log(LAMBDA_DECAY / (level + 1) + 1.0)
        wait_level(level)
        if level + 2 < LAYERS:
            send_level(level + 2)

        def propagate(i, carry):
            g = feat_peer(i, 1)
            lane = lane_ids(TILE)
            agg = jnp.zeros((TILE, LANES), F32)
            for t in range(PACK):
                r = g * PACK + t
                tiles = []
                for k in range(K):
                    column = columns[k, r]
                    tiles.append(comb[level][column >> 2] * masks[column & 3])
                lhs = jnp.concatenate([values[r, k] for k in range(K)], axis=1)
                out = jnp.dot(
                    lhs, jnp.concatenate(tiles, axis=0), preferred_element_type=F32
                )
                out = out + pltpu.roll(out, 64, 1)
                out = out + pltpu.roll(out, 32, 1)
                agg = jnp.where((lane >> 5) == t, out, agg)
            z = (1.0 - ALPHA) * agg + ALPHA * initial[g].astype(F32)
            zs[level, g] = z.astype(BF)
            return carry

        def step(i, carry):
            propagate(i, 0)
            z_copy(level, i - 1).start()
            return carry

        propagate(0, 0)
        lax.fori_loop(1, NFEAT, step, 0)
        zr[level, f_me] = zs[level, f_me]

        def push(part, start):
            pushed[level, :, pl.ds(start, TILE)] = part

        def push_group(g, carry):
            emit_group(level, g, push)
            return carry

        lax.fori_loop(0, GROUPS, push_group, 0)

        def wait_z(i, carry):
            z_copy(level, i).wait_recv()
            return carry

        lax.fori_loop(0, NFEAT - 1, wait_z, 0)

        def mix(half, piece):
            start = pl.multiple_of(half * HALF + piece * 32, 32)
            parts = [zr[level, f, pl.ds(start, 32), :].astype(F32) for f in range(NFEAT)]
            left = swap_blocks(parts[:4])
            right = swap_blocks(parts[4:])
            block = jnp.concatenate(
                [jnp.concatenate([left[t], right[t]], axis=1) for t in range(PACK)], axis=0
            )
            product = jnp.dot(block.astype(BF), weights[level], preferred_element_type=F32)
            fresh = jnp.maximum((1.0 - beta) * block + beta * product, 0.0)
            for a in range(2):
                outs = swap_blocks(
                    [fresh[t * 32:(t + 1) * 32, a * LANES:(a + 1) * LANES] for t in range(PACK)]
                )
                for b in range(PACK):
                    hs[level, a * PACK + b, pl.ds(start, 32), :] = outs[b].astype(BF)

        def mix_half(half, carry):
            mix(half, 0)
            mix(half, 1)

            def send_h(i, inner):
                h_copy(level, half, i).start()
                return inner

            lax.fori_loop(0, NFEAT - 1, send_h, 0)
            return carry

        lax.fori_loop(0, 2, mix_half, 0)
        comb[level + 1][f_me] = hs[level, f_me]

        def drain_dom(k, carry):
            dom_copy(level, k).wait_send()
            return carry

        def drain_z(i, carry):
            z_copy(level, i).wait_send()
            return carry

        lax.fori_loop(0, n_dom - 1, drain_dom, 0)
        lax.fori_loop(0, NFEAT - 1, drain_z, 0)
        if level > 0:
            lax.fori_loop(0, NFEAT - 1, functools.partial(drain_h, level - 1), 0)

        def wait_h(i, carry):
            h_copy(level, 0, i).wait_recv()
            h_copy(level, 1, i).wait_recv()
            return carry

        if level + 1 < LAYERS:
            lax.fori_loop(0, NFEAT - 1, wait_h, 0)

    def finish(part, start):
        final[:, pl.ds(start, TILE)] = part

    def finish_group(i, carry):
        wait_h(i, 0)
        emit_group(LAYERS, feat_peer(i, -1), finish)
        return carry

    emit_group(LAYERS, f_me, finish)
    lax.fori_loop(0, NFEAT - 1, finish_group, 0)

    lax.fori_loop(0, NFEAT - 1, functools.partial(drain_h, LAYERS - 1), 0)


def on_device(
    n_dom, features, w_input, layer_weights, history, tile_values, tile_columns, send_rows, send_counts
):
    grid_x, grid_z = (4, 8) if n_dom == 32 else (1, n_dom)
    table_t = history.transpose(0, 2, 1).reshape(LAYERS * WIDTH, NODES_DEV)
    vmem = pl.BlockSpec(memory_space=pltpu.VMEM)
    smem = pl.BlockSpec(memory_space=pltpu.SMEM)
    hbm = pl.BlockSpec(memory_space=pl.ANY)
    sem = pltpu.SemaphoreType.DMA
    pushed, final = pl.pallas_call(
        functools.partial(layer_kernel, n_dom, grid_x, grid_z),
        out_shape=(
            pltpu.VMEM((LAYERS, WIDTH, NODES_DEV), BF),
            pltpu.VMEM((WIDTH, NODES_DEV), BF),
        ),
        in_specs=[smem, smem, smem, hbm, hbm, vmem, hbm, hbm],
        out_specs=(vmem, vmem),
        scratch_shapes=[
            pltpu.VMEM((LAYERS * WIDTH, NODES_DEV), BF),
            pltpu.VMEM((NODES_DEV + 8, LANES), F32),
            pltpu.VMEM((CAP + 8, LANES), F32),
            pltpu.VMEM((LAYERS, n_dom, TILE, LANES), BF),
            pltpu.VMEM((PACK, TILE, LANES), BF),
            pltpu.VMEM((LANES, PACK * TILE), BF),
            *[pltpu.VMEM((GROUPS + n_dom, TILE, LANES), BF) for _ in range(LAYERS)],
            pltpu.VMEM((GROUPS, TILE, LANES), BF),
            pltpu.VMEM((GROUPS, TILE, LANES), BF),
            pltpu.VMEM((NODES_DEV, LANES), BF),
            pltpu.VMEM((NODES_DEV // TILE, K, TILE, TILE), BF),
            pltpu.VMEM((LAYERS, F, F), BF),
            pltpu.VMEM((LAYERS, NFEAT, TILE, LANES), BF),
            pltpu.VMEM((LAYERS, NFEAT, TILE, LANES), BF),
            pltpu.VMEM((LAYERS, NFEAT, TILE, LANES), BF),
            sem((4,)),
            sem((4,)),
            sem((LAYERS, n_dom - 1)),
            sem((LAYERS, n_dom - 1)),
            sem((LAYERS, NFEAT - 1)),
            sem((LAYERS, NFEAT - 1)),
            sem((LAYERS, 2, NFEAT - 1)),
            sem((LAYERS, 2, NFEAT - 1)),
        ],
        compiler_params=pltpu.CompilerParams(collective_id=0, has_side_effects=True),
        name="halo_layers",
    )(
        tile_columns.T, send_rows.reshape(n_dom // 8, 8, PACK, TILE).transpose(0, 2, 1, 3), send_counts, table_t, features, w_input.T,
        tile_values, layer_weights,
    )
    return pushed.transpose(0, 2, 1), final.transpose(1, 0)


def solution(mesh):
    placed = (
        P("dom", None),
        P(None, "feat"),
        P(),
        P(None, "dom", "feat"),
        P("dom", None, None, None),
        P("dom", None),
        P("dom", None, None),
        P("dom", None),
    )
    return jax.shard_map(
        functools.partial(on_device, mesh.shape["dom"]),
        mesh=mesh,
        in_specs=placed,
        out_specs=(P(None, "dom", "feat"), P("dom", "feat")),
        check_vma=False,
    )
```

```python
import functools
import math

import jax
import jax.numpy as jnp
from jax import lax
from jax.experimental import pallas as pl
from jax.experimental.pallas import tpu as pltpu
from jax.sharding import PartitionSpec as P

MESH = pl.DeviceIdType.MESH
LAYERS = 4
ALPHA = 0.1
LAMBDA_DECAY = 0.5
TILE = 128
HALF = 64
LANES = 128
PACK = 4
WIDTH = 32
NFEAT = 8
GROUPS = 8
CAP = 512
NODES_DEV = 4096
F = 256
K = 6
BF = jnp.bfloat16
F32 = jnp.float32


def lane_ids(rows):
    return lax.broadcasted_iota(jnp.int32, (rows, LANES), 1)


def swap_blocks(parts):
    x0, x1, x2, x3 = parts
    lane = lane_ids(x0.shape[0])
    low = lane < 64
    even = (lane & 32) == 0
    a0 = jnp.where(low, x0, pltpu.roll(x2, 64, 1))
    a2 = jnp.where(low, pltpu.roll(x0, 64, 1), x2)
    a1 = jnp.where(low, x1, pltpu.roll(x3, 64, 1))
    a3 = jnp.where(low, pltpu.roll(x1, 64, 1), x3)
    y0 = jnp.where(even, a0, pltpu.roll(a1, 32, 1))
    y1 = jnp.where(even, pltpu.roll(a0, 96, 1), a1)
    y2 = jnp.where(even, a2, pltpu.roll(a3, 32, 1))
    y3 = jnp.where(even, pltpu.roll(a2, 96, 1), a3)
    return y0, y1, y2, y3


def fill_table(table_t, table, piece):
    def block(i, carry):
        for u in range(4):
            start = pl.multiple_of((piece * 8 + i * 4 + u) * TILE, TILE)
            table[pl.ds(start, TILE), :] = table_t[:, pl.ds(start, TILE)].T.astype(F32)
        return carry

    lax.fori_loop(0, 2, block, 0)


def gather_rows(rows, table, picked, dest):
    high, low = dest // 8, dest % 8
    for t in range(PACK):
        for i in range(TILE):
            picked[pl.ds(t * TILE + i, 1), :] = table[pl.ds(rows[high, t, low, i], 1), :]


def pack_rows(counts, picked, packed, dest):
    row = lax.broadcasted_iota(jnp.int32, (32, LANES), 0)
    count = counts[0, dest]
    for c in range(4):
        parts = []
        for t in range(PACK):
            start = t * TILE + c * 32
            live = row < count - start
            parts.append(jnp.where(live, picked[pl.ds(start, 32), :], 0.0))
        for level, part in enumerate(swap_blocks(parts)):
            packed[level, dest, pl.ds(c * 32, 32), :] = part.astype(BF)


def layer_kernel(
    n_dom, grid_x, grid_z,
    columns, rows, counts, table_hbm, feats_hbm, w_in_t, values_hbm, weights_hbm,
    pushed,
    table_t, table, picked, packed, masks, w_wide,
    comb0, comb1, comb2, comb3, last, initial, feats, values, weights, zs, zr, hs,
    table_sem, load_sem, dom_send, dom_recv, z_send, z_recv, h_send, h_recv,
):
    comb = (comb0, comb1, comb2, comb3, last)
    f_me = lax.axis_index("feat")
    d_me = lax.axis_index("dom")
    x_me, z_me = d_me // grid_z, d_me % grid_z

    def load_table(piece):
        part = pl.ds(piece * (NODES_DEV // 4), NODES_DEV // 4)
        return pltpu.make_async_copy(
            table_hbm.at[:, part], table_t.at[:, part], table_sem.at[piece]
        )

    for piece in range(4):
        load_table(piece).start()

    barrier = pltpu.get_barrier_semaphore()

    def greet_dom(i, carry):
        pl.semaphore_signal(
            barrier, inc=1, device_id=(f_me, lax.rem(d_me + 1 + i, n_dom)), device_id_type=MESH
        )
        return carry

    def feat_peer(i, sign):
        pair, odd = i // 2, lax.rem(i, 2)
        step = jnp.where(pair == 0, 2, jnp.where(pair == 1, 1, jnp.where(pair == 2, 3, 0)))
        flip = jnp.where(pair == 3, 1 - odd, odd)
        chip = lax.rem(f_me // 2 + 4 + sign * step, 4)
        return chip * 2 + lax.rem(f_me + flip, 2)

    def greet_feat(i, carry):
        pl.semaphore_signal(
            barrier, inc=1, device_id=(feat_peer(i, 1), d_me), device_id_type=MESH
        )
        return carry

    lax.fori_loop(0, n_dom - 1, greet_dom, 0)
    lax.fori_loop(0, NFEAT - 1, greet_feat, 0)
    load_feats = pltpu.make_async_copy(feats_hbm, feats, load_sem.at[1])
    load_values = pltpu.make_async_copy(values_hbm, values, load_sem.at[2])
    load_weights = pltpu.make_async_copy(weights_hbm, weights, load_sem.at[3])
    load_feats.start()
    load_values.start()
    load_weights.start()
    lane = lane_ids(TILE)
    for b in range(PACK):
        masks[b] = jnp.where((lane >> 5) == b, 1.0, 0.0).astype(BF)
    w_wide[...] = jnp.zeros((LANES, PACK * TILE), BF)
    for t in range(PACK):
        w_wide[t * WIDTH:(t + 1) * WIDTH, t * TILE:(t + 1) * TILE] = w_in_t[...]
    for piece in range(4):
        load_table(piece).wait()
        fill_table(table_t, table, piece)

    def dest_of(k):
        i = lax.rem(k, grid_z)
        half = grid_z // 2
        dz = jnp.where(lax.rem(i, 2) == 1, half - (i + 1) // 2, half + i // 2)
        dx = lax.rem(grid_x - 1 - k // grid_z + i + 1, grid_x)
        return lax.rem(x_me + dx, grid_x) * grid_z + lax.rem(z_me + dz, grid_z)

    def dom_copy(level, k):
        dest = dest_of(k)
        return pltpu.make_async_remote_copy(
            src_ref=packed.at[level, dest],
            dst_ref=comb[level].at[GROUPS + d_me],
            send_sem=dom_send.at[level, k],
            recv_sem=dom_recv.at[level, k],
            device_id=(f_me, dest),
            device_id_type=MESH,
        )

    def send_level(level):
        def one(k, carry):
            dom_copy(level, k).start()
            return carry

        lax.fori_loop(0, n_dom - 1, one, 0)

    def wait_level(level):
        def one(k, carry):
            dom_copy(level, k).wait_recv()
            return carry

        lax.fori_loop(0, n_dom - 1, one, 0)

    def z_copy(level, i):
        dest = feat_peer(i, 1)
        return pltpu.make_async_remote_copy(
            src_ref=zs.at[level, dest],
            dst_ref=zr.at[level, f_me],
            send_sem=z_send.at[level, i],
            recv_sem=z_recv.at[level, i],
            device_id=(dest, d_me),
            device_id_type=MESH,
        )

    def h_copy(level, half, i):
        dest = feat_peer(i, 1)
        part = pl.ds(pl.multiple_of(half * HALF, HALF), HALF)
        return pltpu.make_async_remote_copy(
            src_ref=hs.at[level, dest, part],
            dst_ref=comb[level + 1].at[f_me, part],
            send_sem=h_send.at[level, half, i],
            recv_sem=h_recv.at[level, half, i],
            device_id=(dest, d_me),
            device_id_type=MESH,
        )

    def gather(k, carry):
        dest = dest_of(k)
        gather_rows(rows, table, picked, dest)
        pack_rows(counts, picked, packed, dest)
        return carry

    def gather_step(k, carry):
        gather(k, 0)
        dom_copy(0, k - 1).start()
        return carry

    def send_first(k, carry):
        dom_copy(0, k).start()
        return carry

    ahead = min(2, n_dom - 1)
    lax.fori_loop(0, ahead, gather, 0)
    pl.semaphore_wait(barrier, n_dom - 1 + NFEAT - 1)
    lax.fori_loop(0, ahead - 1, send_first, 0)
    lax.fori_loop(ahead, n_dom - 1, gather_step, 0)
    for level in range(LAYERS):
        comb[level][GROUPS + d_me] = jnp.zeros((TILE, LANES), BF)

    dom_copy(0, n_dom - 2).start()
    send_level(1)
    load_feats.wait()

    def start_group(g, carry):
        for c in range(2):
            own = [
                feats[pl.ds(pl.multiple_of((g * PACK + t) * TILE + c * 64, 64), 64), :]
                for t in range(PACK)
            ]
            h0 = lax.dot_general(
                jnp.concatenate(own, axis=1), w_wide[...], (((1,), (1,)), ((), ())),
                preferred_element_type=F32,
            )
            h0 = jnp.maximum(h0, 0.0).astype(BF)
            comb0[g, pl.ds(c * 64, 64), :] = h0
            initial[g, pl.ds(c * 64, 64), :] = h0
        return carry

    lax.fori_loop(0, GROUPS, start_group, 0)
    load_values.wait()
    load_weights.wait()

    def emit_group(level, g, target):
        flipped = comb[level][g].T
        for t in range(PACK):
            start = pl.multiple_of((g * PACK + t) * TILE, TILE)
            target(flipped[t * WIDTH:(t + 1) * WIDTH], start)

    def drain_h(level, i, carry):
        h_copy(level, 0, i).wait_send()
        h_copy(level, 1, i).wait_send()
        return carry

    for level in range(LAYERS):
        beta = math.log(LAMBDA_DECAY / (level + 1) + 1.0)
        wait_level(level)
        if level + 2 < LAYERS:
            send_level(level + 2)

        def propagate(i, carry):
            g = feat_peer(i, 1)
            lane = lane_ids(TILE)
            agg = jnp.zeros((TILE, LANES), F32)
            for t in range(PACK):
                r = g * PACK + t
                tiles = []
                for k in range(K):
                    column = columns[k, r]
                    tiles.append(comb[level][column >> 2] * masks[column & 3])
                lhs = jnp.concatenate([values[r, k] for k in range(K)], axis=1)
                out = jnp.dot(
                    lhs, jnp.concatenate(tiles, axis=0), preferred_element_type=F32
                )
                out = out + pltpu.roll(out, 64, 1)
                out = out + pltpu.roll(out, 32, 1)
                agg = jnp.where((lane >> 5) == t, out, agg)
            z = (1.0 - ALPHA) * agg + ALPHA * initial[g].astype(F32)
            zs[level, g] = z.astype(BF)
            return carry

        def step(i, carry):
            propagate(i, 0)
            z_copy(level, i - 1).start()
            return carry

        propagate(0, 0)
        lax.fori_loop(1, NFEAT, step, 0)
        zr[level, f_me] = zs[level, f_me]

        def push(part, start):
            pushed[level, :, pl.ds(start, TILE)] = part

        def push_group(g, carry):
            emit_group(level, g, push)
            return carry

        lax.fori_loop(0, GROUPS, push_group, 0)

        def wait_z(i, carry):
            z_copy(level, i).wait_recv()
            return carry

        lax.fori_loop(0, NFEAT - 1, wait_z, 0)

        def mix(half, piece):
            start = pl.multiple_of(half * HALF + piece * 32, 32)
            parts = [zr[level, f, pl.ds(start, 32), :].astype(F32) for f in range(NFEAT)]
            left = swap_blocks(parts[:4])
            right = swap_blocks(parts[4:])
            block = jnp.concatenate(
                [jnp.concatenate([left[t], right[t]], axis=1) for t in range(PACK)], axis=0
            )
            product = jnp.dot(block.astype(BF), weights[level], preferred_element_type=F32)
            fresh = jnp.maximum((1.0 - beta) * block + beta * product, 0.0)
            for a in range(2):
                outs = swap_blocks(
                    [fresh[t * 32:(t + 1) * 32, a * LANES:(a + 1) * LANES] for t in range(PACK)]
                )
                for b in range(PACK):
                    hs[level, a * PACK + b, pl.ds(start, 32), :] = outs[b].astype(BF)

        def mix_half(half, carry):
            mix(half, 0)
            mix(half, 1)

            def send_h(i, inner):
                h_copy(level, half, i).start()
                return inner

            lax.fori_loop(0, NFEAT - 1, send_h, 0)
            return carry

        lax.fori_loop(0, 2, mix_half, 0)
        comb[level + 1][f_me] = hs[level, f_me]

        def drain_dom(k, carry):
            dom_copy(level, k).wait_send()
            return carry

        def drain_z(i, carry):
            z_copy(level, i).wait_send()
            return carry

        lax.fori_loop(0, n_dom - 1, drain_dom, 0)
        lax.fori_loop(0, NFEAT - 1, drain_z, 0)
        if level > 0:
            lax.fori_loop(0, NFEAT - 1, functools.partial(drain_h, level - 1), 0)

        def wait_h(i, carry):
            h_copy(level, 0, i).wait_recv()
            h_copy(level, 1, i).wait_recv()
            return carry

        if level + 1 < LAYERS:
            lax.fori_loop(0, NFEAT - 1, wait_h, 0)

    def finish(part, start):
        pushed[LAYERS, :, pl.ds(start, TILE)] = part

    def finish_group(i, carry):
        wait_h(i, 0)
        emit_group(LAYERS, feat_peer(i, -1), finish)
        return carry

    emit_group(LAYERS, f_me, finish)
    lax.fori_loop(0, NFEAT - 1, finish_group, 0)

    lax.fori_loop(0, NFEAT - 1, functools.partial(drain_h, LAYERS - 1), 0)


def on_device(
    n_dom, features, w_input, layer_weights, history, tile_values, tile_columns, send_rows, send_counts
):
    grid_x, grid_z = (4, 8) if n_dom == 32 else (1, n_dom)
    table_t = history.transpose(0, 2, 1).reshape(LAYERS * WIDTH, NODES_DEV)
    vmem = pl.BlockSpec(memory_space=pltpu.VMEM)
    smem = pl.BlockSpec(memory_space=pltpu.SMEM)
    hbm = pl.BlockSpec(memory_space=pl.ANY)
    sem = pltpu.SemaphoreType.DMA
    (rows_t,) = pl.pallas_call(
        functools.partial(layer_kernel, n_dom, grid_x, grid_z),
        out_shape=(
            pltpu.VMEM((LAYERS + 1, WIDTH, NODES_DEV), BF),
        ),
        in_specs=[smem, smem, smem, hbm, hbm, vmem, hbm, hbm],
        out_specs=(vmem,),
        scratch_shapes=[
            pltpu.VMEM((LAYERS * WIDTH, NODES_DEV), BF),
            pltpu.VMEM((NODES_DEV, LANES), F32),
            pltpu.VMEM((CAP, LANES), F32),
            pltpu.VMEM((LAYERS, n_dom, TILE, LANES), BF),
            pltpu.VMEM((PACK, TILE, LANES), BF),
            pltpu.VMEM((LANES, PACK * TILE), BF),
            *[pltpu.VMEM((GROUPS + n_dom, TILE, LANES), BF) for _ in range(LAYERS)],
            pltpu.VMEM((GROUPS, TILE, LANES), BF),
            pltpu.VMEM((GROUPS, TILE, LANES), BF),
            pltpu.VMEM((NODES_DEV, LANES), BF),
            pltpu.VMEM((NODES_DEV // TILE, K, TILE, TILE), BF),
            pltpu.VMEM((LAYERS, F, F), BF),
            pltpu.VMEM((LAYERS, NFEAT, TILE, LANES), BF),
            pltpu.VMEM((LAYERS, NFEAT, TILE, LANES), BF),
            pltpu.VMEM((LAYERS, NFEAT, TILE, LANES), BF),
            sem((4,)),
            sem((4,)),
            sem((LAYERS, n_dom - 1)),
            sem((LAYERS, n_dom - 1)),
            sem((LAYERS, NFEAT - 1)),
            sem((LAYERS, NFEAT - 1)),
            sem((LAYERS, 2, NFEAT - 1)),
            sem((LAYERS, 2, NFEAT - 1)),
        ],
        compiler_params=pltpu.CompilerParams(collective_id=0, has_side_effects=True),
        name="halo_layers",
    )(
        tile_columns.T, send_rows.reshape(n_dom // 8, 8, PACK, TILE).transpose(0, 2, 1, 3), send_counts, table_t, features, w_input.T,
        tile_values, layer_weights,
    )
    return rows_t[:LAYERS].transpose(0, 2, 1), rows_t[LAYERS].transpose(1, 0)


def solution(mesh):
    placed = (
        P("dom", None),
        P(None, "feat"),
        P(),
        P(None, "dom", "feat"),
        P("dom", None, None, None),
        P("dom", None),
        P("dom", None, None),
        P("dom", None),
    )
    return jax.shard_map(
        functools.partial(on_device, mesh.shape["dom"]),
        mesh=mesh,
        in_specs=placed,
        out_specs=(P(None, "dom", "feat"), P("dom", "feat")),
        check_vma=False,
    )
```
